128 devices in a mesh: pages: 16 (over y, x_hi, core), heads: 8 (over x_lo, z).
Axes of the slice: x: 4 (x_hi: 2, x_lo: 2; x = x_hi * 2 + x_lo), y: 4, z: 4, core: 2. Of those that a mesh axis runs over, the one named last changes fastest.
Arguments:
- queries: bfloat16 [1024, 32, 128], P('pages', 'heads'), may hold values from -6 to 6
- keys: bfloat16 [1152, 16, 128, 128], P('pages', 'heads'), may hold values from -6 to 6
- values: bfloat16 [1152, 16, 128, 128], P('pages', 'heads'), may hold values from -6 to 6
- hot_pages: int32 [64], replicated, may hold values from 0 to 1151, as said below
- hot_used: int32 [1024], replicated, may hold values from 1 to 64
- user_pages: int32 [1024, 1], P('pages'), may hold values from 8 to 71, as said below
- lengths: int32 [1024], P('pages'), may hold values from 1 to 128
- o_weight: bfloat16 [4096, 4608], P('heads'), may hold values from -0.09375 to 0.09375
- residual: bfloat16 [1024, 4608], P(('pages', 'heads')), may hold values from -6 to 6
- norm_gain: float32 [4608], replicated, may hold values from 0.25 to 1.75
Outputs:
- output: bfloat16 [1024, 4608], P(('pages', 'heads'))
The draws below stay inside these ranges and needn't reach their ends.
Inputs may be any that keep to these rules, and one draw needn't show every extreme that they name: `hot_pages`: 64 distinct pages; each lies among the first 8 pages of its group (page p belongs to group p // 72); one group holds exactly 8 of them and none holds more. `user_pages`: numbers within the sequence's own group (sequence s belongs to group s // 64); all own pages of the sequences of one group are distinct.
All inputs are finite; a program needn't handle non-finite values.
Results may differ from the reference program's by a relative error of at most 0.019.
Values may be sent and summed in bfloat16 or wider, within the bound.
A program may use at most 128 MiB of HBM per device.

```python
import jax
import jax.numpy as jnp
from jax import lax

DM = 4608
QH = 32
KVH = 16
HD = 128
PAGE = 128
HOT = 64
HOT_CAP = 8
UPS = 1
SEQ_DEV = 64
PG_DEV = 72
GROUPS = 16
PAGES = 1152
SEQS = 1024


def draw_hot_pages(key, part):
    key_full, key_rank, key_order = jax.random.split(jax.random.fold_in(key, 11), 3)
    slot_ids = jnp.arange(GROUPS * HOT_CAP, dtype=jnp.int32)
    group_of = slot_ids // HOT_CAP
    within = slot_ids % HOT_CAP
    full_group = jax.random.randint(key_full, (), 0, GROUPS, dtype=jnp.int32)
    ranking = jax.random.permutation(key_rank, GROUPS * HOT_CAP).astype(jnp.int32)
    priority = jnp.where(group_of == full_group, within - HOT_CAP, ranking)
    chosen = jnp.argsort(priority, stable=True)[:HOT]
    picked = (group_of * PG_DEV + within)[chosen]
    return jax.random.permutation(key_order, picked).astype(jnp.int32)


def draw_user_pages(key, part):
    group_keys = jax.random.split(jax.random.fold_in(key, 23), GROUPS)

    def one_group(group_key):
        return jax.random.permutation(group_key, PG_DEV - HOT_CAP)[:SEQ_DEV * UPS].astype(jnp.int32)
    picked = jax.vmap(one_group)(group_keys) + HOT_CAP
    return picked.reshape(SEQS, UPS).astype(jnp.int32)


def place_ends(entries, key, smallest, high):
    longest = entries.shape.index(max(entries.shape))
    spots = []
    for shift in (0, 1):
        where = [jax.random.randint(jax.random.fold_in(key, axis), (), 0, length) for axis, length in enumerate(entries.shape)]
        where[longest] = (where[longest] + shift) % entries.shape[longest]
        spots.append(tuple(where))
    return entries.at[spots[0]].set(smallest).at[spots[1]].set(high)


def block_levels(own_key, dims, shards, least, top_value):
    loudness = 1.0
    for position, shards_of in shards:
        draws = jax.random.uniform(jax.random.fold_in(jax.random.fold_in(own_key, 6), position), (shards_of,), jnp.float32, least / len(shards), top_value / len(shards))
        loudness = loudness * jnp.repeat(jnp.exp(draws), dims[position] // shards_of).reshape((-1,) + (1,) * (len(dims) - 1 - position))
    return loudness


def normal_values(stream_key, shape, spread, most, shards=(), kind=jnp.bfloat16):
    array = jax.random.normal(stream_key, shape, jnp.float32) * spread
    if len(shards) > 0:
        array = block_levels(stream_key, shape, shards, -0.22, 0.18) * array
    return jnp.clip(array, min=-most, max=most).astype(kind)


def setup_inputs(seed: int = 0) -> dict:
    arg_keys = jax.random.split(jax.random.key(seed), 11)
    return {
        "queries": normal_values(arg_keys[0], (SEQS, QH, HD), 1.0, 6.0, ((0, 16), (1, 8))),
        "keys": normal_values(arg_keys[1], (PAGES, KVH, PAGE, HD), 1.0, 6.0, ((0, 16), (1, 8))),
        "values": normal_values(arg_keys[2], (PAGES, KVH, PAGE, HD), 1.0, 6.0, ((0, 16), (1, 8))),
        "hot_pages": draw_hot_pages(jax.random.fold_in(arg_keys[10], 71), 0),
        "hot_used": place_ends(jax.random.randint(arg_keys[4], (SEQS,), 1, HOT + 1), jax.random.fold_in(arg_keys[4], 1), 1, HOT).astype(jnp.int32),
        "user_pages": draw_user_pages(jax.random.fold_in(arg_keys[10], 71), 0),
        "lengths": place_ends(jax.random.randint(arg_keys[6], (SEQS,), 1, UPS * PAGE + 1), jax.random.fold_in(arg_keys[6], 1), 1, UPS * PAGE).astype(jnp.int32),
        "o_weight": normal_values(arg_keys[7], (QH * HD, DM), (QH * HD) ** -0.5, 0.09375, ((0, 8),)),
        "residual": normal_values(arg_keys[8], (SEQS, DM), 1.0, 6.0, ((0, 128),)),
        "norm_gain": jnp.clip(1.0 + 0.15 * jax.random.normal(arg_keys[9], (DM,), jnp.float32), 0.25, 1.75),
    }


score_scale = 1.0 / 12.0
soft_cap = 50.0
epsilon = 1e-06

def reference(queries, keys, values, hot_pages, hot_used, user_pages, lengths, o_weight, residual, norm_gain):
    group_size = QH // KVH
    seq_total = queries.shape[0]
    owner_base = jnp.arange(seq_total, dtype=jnp.int32) // SEQ_DEV * PG_DEV
    user_ids = (owner_base[:, None] + user_pages).astype(jnp.int32)
    hot_token_page = jnp.arange(HOT * PAGE, dtype=jnp.int32) // PAGE
    hot_mask = hot_token_page[None, :] < hot_used[:, None]
    user_mask = jnp.arange(UPS * PAGE, dtype=jnp.int32)[None, :] < lengths[:, None]

    def weights_of(logits, allowed):
        weight = jnp.exp(soft_cap * jnp.tanh(logits * score_scale / soft_cap))
        weight = jnp.where(allowed, weight, jnp.float32(0.0))
        rounded = lax.optimization_barrier(weight.astype(jnp.bfloat16))
        return (weight, rounded.astype(jnp.float32))

    def per_head(kv_index):
        query_f32 = lax.dynamic_slice_in_dim(queries, kv_index * group_size, group_size, 1).astype(jnp.float32)
        hot_keys = keys[hot_pages, kv_index].reshape(HOT * PAGE, HD).astype(jnp.float32)
        hot_values = values[hot_pages, kv_index].reshape(HOT * PAGE, HD).astype(jnp.float32)
        own_keys = keys[user_ids, kv_index].reshape(seq_total, UPS * PAGE, HD).astype(jnp.float32)
        own_values = values[user_ids, kv_index].reshape(seq_total, UPS * PAGE, HD).astype(jnp.float32)
        hot_logits = jnp.einsum('sgd,td->sgt', query_f32, hot_keys)
        hot_weight, hot_rounded = weights_of(hot_logits, hot_mask[:, None, :])
        own_logits = jnp.einsum('sgd,std->sgt', query_f32, own_keys)
        own_weight, own_rounded = weights_of(own_logits, user_mask[:, None, :])
        numerator = jnp.einsum('sgt,td->sgd', hot_rounded, hot_values) + jnp.einsum('sgt,std->sgd', own_rounded, own_values)
        totals = lax.optimization_barrier(jnp.sum(hot_weight, axis=2)) + lax.optimization_barrier(jnp.sum(own_weight, axis=2))
        return (numerator / totals[:, :, None]).astype(jnp.bfloat16)
    per_kv = lax.map(per_head, jnp.arange(KVH, dtype=jnp.int32))
    attended = jnp.transpose(per_kv, (1, 0, 2, 3)).reshape(seq_total, QH * HD)
    projected = jnp.dot(attended, o_weight, preferred_element_type=jnp.float32)
    mean_sq = lax.optimization_barrier(jnp.mean(projected * projected, axis=1, keepdims=True))
    normed = projected / jnp.sqrt(mean_sq + epsilon) * norm_gain[None, :]
    return (residual.astype(jnp.float32) + normed).astype(jnp.bfloat16)
```

```python
import functools
import math

import jax
import jax.numpy as jnp
from jax import lax
from jax.experimental import pallas as pl
from jax.experimental.pallas import tpu as pltpu
from jax.sharding import PartitionSpec as P

HOT_CAP = 8
soft_cap = 50.0
score_scale = 1.0 / 12.0
epsilon = 1e-06
NY = 4
F32, BF16, I32 = jnp.float32, jnp.bfloat16, jnp.int32
MESH = pl.DeviceIdType.MESH

A0, A3, A1, A2, B3, B1, B2, B0 = range(8)
OWNER = {A0: (0, 0), A3: (3, 0), A1: (1, 0), A2: (2, 0), B3: (3, 1), B1: (1, 1), B2: (2, 1), B0: (0, 1)}


def weights_of(logits):
    return jnp.exp2(jnp.tanh(logits * (score_scale / soft_cap)) * (soft_cap * math.log2(math.e)))


def split_sum(totals, rows):
    high = totals.astype(BF16).astype(F32)
    row = lax.broadcasted_iota(I32, (16, rows), 0)
    return jnp.where(row == 0, high, jnp.where(row == 1, totals - high, 0.0)).astype(BF16)


def attention_kernel(
    q_hbm, k_hbm, v_hbm, hot_hbm, used_hbm, up_hbm, len_hbm, out_ref,
    q_v, hot_v, used_v, len_v, up_s, kbuf, vbuf, hk, hv, vt, qt, qbd, wt, urow, lrow, pos,
    res, ra, rb, rx, bsum, own_t, own_w, own_o,
    in_sem, kv_send, kv_recv, ag_send, ag_recv, rs_send, rs_recv,
):
    seqs = len_v.shape[1]
    kvh, page, hd = hk.shape[1:]
    rows = q_v.shape[0]
    half = rows // kvh
    me = lax.axis_index("pages")
    y, xh, core = me // 4, (me // 2) % 2, me % 2

    def at(dy, dx=0, dc=0):
        return {"pages": ((y + dy) % NY) * 4 + ((xh + dx) % 2) * 2 + (core + dc) % 2}

    def remote(src, dst, send, recv, target):
        return pltpu.make_async_remote_copy(
            src_ref=src, dst_ref=dst, send_sem=send, recv_sem=recv, device_id=target, device_id_type=MESH
        )

    local = [
        pltpu.make_async_copy(q_hbm, q_v, in_sem.at[0]),
        pltpu.make_async_copy(hot_hbm, hot_v, in_sem.at[1]),
        pltpu.make_async_copy(used_hbm, used_v, in_sem.at[2]),
        pltpu.make_async_copy(len_hbm, len_v, in_sem.at[3]),
        pltpu.make_async_copy(up_hbm, up_s, in_sem.at[4]),
        pltpu.make_async_copy(v_hbm.at[pl.ds(0, HOT_CAP)], hv.at[pl.ds(0, HOT_CAP)], in_sem.at[5]),
        pltpu.make_async_copy(k_hbm.at[pl.ds(0, HOT_CAP)], hk.at[pl.ds(0, HOT_CAP)], in_sem.at[6]),
        pltpu.make_async_copy(k_hbm, kbuf, in_sem.at[7]),
        pltpu.make_async_copy(v_hbm, vbuf, in_sem.at[8]),
    ]
    for copy in local:
        copy.start()

    barrier = pltpu.get_barrier_semaphore()
    peers = [at(1), at(2), at(3), at(0, 1), at(0, 0, 1)]
    for peer in peers:
        pl.semaphore_signal(barrier, inc=1, device_id=peer, device_id_type=MESH)

    local[0].wait()
    r = lax.broadcasted_iota(I32, (rows, rows), 0)
    col = lax.broadcasted_iota(I32, (rows, rows), 1)
    heads = rows // seqs
    perm = jnp.where(col == (r % seqs) * heads + r // seqs, 1.0, 0.0).astype(BF16)
    q_rows = jnp.dot(perm, q_v[...], preferred_element_type=F32)
    qt[A0] = q_rows.T.astype(BF16)

    pl.semaphore_wait(barrier, len(peers))

    kv_copies = [
        remote(k_hbm.at[pl.ds(0, HOT_CAP)], hk.at[pl.ds(HOT_CAP, HOT_CAP)], kv_send.at[0], kv_recv.at[0], at(0, 0, 1)),
        remote(v_hbm.at[pl.ds(0, HOT_CAP)], hv.at[pl.ds(HOT_CAP, HOT_CAP)], kv_send.at[1], kv_recv.at[1], at(0, 0, 1)),
    ]
    plan = [(A0, B0, (0, 1)), (A0, A3, (1, 0)), (A0, A1, (3, 0)), (A3, A2, (1, 0)), (B0, B3, (1, 0)), (B0, B1, (3, 0)), (B1, B2, (3, 0))]
    gathers = {
        dst: remote(qt.at[src], qt.at[dst], ag_send.at[k], ag_recv.at[k], at(*to))
        for k, (src, dst, to) in enumerate(plan)
    }
    returns = {}
    for k, step in enumerate((A3, A1, A2, B3, B1, B2)):
        dy, dx = OWNER[step]
        slots = rb if dx else ra
        returns[step] = remote(res.at[step], slots.at[NY - dy - 1], rs_send.at[k], rs_recv.at[k], at(dy))
    cross = remote(bsum, rx, rs_send.at[6], rs_recv.at[6], at(0, 1))

    gathers[B0].start()
    gathers[A3].start()
    gathers[A1].start()
    for copy in kv_copies:
        copy.start()

    for copy in local[1:5]:
        copy.wait()
    lane = lax.broadcasted_iota(I32, (2 * seqs, rows), 0)
    pick = lax.broadcasted_iota(I32, (2 * seqs, rows), 1) % seqs
    spread = jnp.where(lane == core * seqs + pick, 1.0, 0.0).astype(BF16)
    used = jnp.dot(used_v[...].astype(F32).astype(BF16), spread, preferred_element_type=F32)
    own_t[pl.ds(0, 8), :] = used
    for step, (dy, dx) in OWNER.items():
        chip = ((y + dy) % NY) * 2 + (xh + dx) % 2
        urow[pl.ds(step, 1), :] = own_t[pl.ds(chip, 1), :]
    lane = lax.broadcasted_iota(I32, (seqs, rows), 0)
    pick = lax.broadcasted_iota(I32, (seqs, rows), 1) % seqs
    spread = jnp.where(lane == pick, 1.0, 0.0).astype(BF16)
    lens = jnp.broadcast_to(len_v[...].astype(F32), (8, seqs)).astype(BF16)
    lrow[...] = jnp.dot(lens, spread, preferred_element_type=F32)
    hot_n = hot_v.shape[1]
    cand = lax.broadcasted_iota(I32, (2 * HOT_CAP, hot_n), 0)
    group = jnp.where(cand < HOT_CAP, me, at(0, 0, 1)["pages"])
    match = hot_v[...] == group * k_hbm.shape[0] + cand % HOT_CAP
    order = lax.broadcasted_iota(I32, (2 * HOT_CAP, hot_n), 1).astype(F32)
    pos[...] = jnp.broadcast_to(
        jnp.min(jnp.where(match, order, 1e9), axis=1, keepdims=True), pos.shape
    )

    qbd[...] = jnp.zeros_like(qbd)

    def set_queries(step):
        qbd[0, pl.ds(0, hd), pl.ds(0, half)] = qt[step, :, pl.ds(0, half)]
        qbd[0, pl.ds(hd, hd), pl.ds(half, half)] = qt[step, :, pl.ds(half, half)]

    def transpose_values(first):
        for j in range(first, first + HOT_CAP):
            for h in range(kvh):
                vt[h, :, pl.ds(j * page, page)] = hv[j, h].T

    local[5].wait()
    transpose_values(0)
    local[6].wait()

    def shared_block(step):
        set_queries(step)
        allowed = jnp.where(urow[pl.ds(step, 1), :] > pos[:, pl.ds(0, 1)], 1.0, 0.0)
        total = jnp.zeros((1, rows), F32)
        parts = [jnp.zeros((hd, half), F32) for _ in range(kvh)]
        for c in range(HOT_CAP):
            keys = jnp.concatenate(
                [hk[pl.ds(2 * c, 2), h].reshape(2 * page, hd) for h in range(kvh)], axis=1
            )
            logits = jnp.dot(keys, qbd[0], preferred_element_type=F32)
            weight = weights_of(logits)
            weight = jnp.concatenate(
                [weight[i * page : (i + 1) * page] * allowed[2 * c + i : 2 * c + i + 1] for i in range(2)], axis=0
            )
            total = total + jnp.sum(weight, axis=0, keepdims=True)
            rounded = weight.astype(BF16)
            for h in range(kvh):
                parts[h] = parts[h] + jnp.dot(
                    vt[h, :, pl.ds(2 * c * page, 2 * page)],
                    rounded[:, h * half : (h + 1) * half],
                    preferred_element_type=F32,
                )
        for h in range(kvh):
            res[step, pl.ds(0, hd), pl.ds(h * half, half)] = parts[h].astype(BF16)
        res[step, pl.ds(hd, 16), :] = split_sum(total, rows)

    def own_scores():
        local[7].wait()
        set_queries(A0)

        def four(g, carry):
            seq_of = lax.broadcasted_iota(I32, (page, rows), 1) % seqs
            tile = own_t[...]
            for i in range(0, 4, 2):
                pages = [up_s[0, g * 4 + i + j] for j in range(2)]
                keys = jnp.concatenate(
                    [jnp.concatenate([kbuf[u, h] for h in range(kvh)], axis=1) for u in pages], axis=0
                )
                logits = jnp.dot(keys, qbd[0], preferred_element_type=F32)
                for j in range(2):
                    tile = jnp.where(seq_of == g * 4 + i + j, logits[j * page : (j + 1) * page], tile)
            own_t[...] = tile
            return carry

        own_t[...] = jnp.zeros_like(own_t)
        lax.fori_loop(0, seqs // 4, four, 0)
        token = lax.broadcasted_iota(I32, (page, rows), 0).astype(F32)
        weight = jnp.where(token < lrow[pl.ds(0, 1), :], weights_of(own_t[...]), 0.0)
        own_t[pl.ds(0, 8), :] = jnp.broadcast_to(jnp.sum(weight, axis=0, keepdims=True), (8, rows))
        own_w[...] = weight.T

    def own_values():
        local[8].wait()
        own_o[...] = jnp.zeros_like(own_o)

        def eight(g, carry):
            seq_of = lax.broadcasted_iota(I32, (rows, page), 0) % seqs
            left, right = [], []
            for i in range(8):
                u = up_s[0, g * 8 + i]
                left.append(jnp.where(seq_of == g * 8 + i, own_w[...], 0.0).astype(BF16))
                right.append(jnp.concatenate([vbuf[u, h] for h in range(kvh)], axis=1))
            own_o[...] += jnp.dot(
                jnp.concatenate(left, axis=1), jnp.concatenate(right, axis=0), preferred_element_type=F32
            )
            return carry

        lax.fori_loop(0, seqs // 8, eight, 0)

    own_scores()
    kv_copies[0].wait()
    kv_copies[1].wait()
    transpose_values(HOT_CAP)

    def one_step(step, carry):
        for k in (A3, A1, A2, B3, B1, B2):
            @pl.when(step == k)
            def _():
                gathers[k].wait_recv()

        @pl.when(step == A3)
        def _():
            gathers[A2].start()

        @pl.when(step == A1)
        def _():
            gathers[B0].wait_recv()
            gathers[B3].start()
            gathers[B1].start()

        @pl.when(step == B1)
        def _():
            gathers[B2].start()

        shared_block(step)
        for k in (A3, A1, A2, B3, B1, B2):
            @pl.when(step == k)
            def _():
                returns[k].start()
        return carry

    lax.fori_loop(0, 8, one_step, 0)
    own_values()

    def summed(pieces):
        return sum(piece[...].astype(F32) for piece in pieces)

    for step in (B3, B1, B2):
        returns[step].wait_recv()
    whole = summed([res.at[B0], rb.at[0], rb.at[1], rb.at[2]])
    bsum[pl.ds(0, hd), :] = whole[:hd].astype(BF16)
    bsum[pl.ds(hd, 16), :] = split_sum(jnp.sum(whole[hd:], axis=0, keepdims=True), rows)
    cross.start()
    own_num = [own_o[pl.ds(h * half, half), pl.ds(h * hd, hd)].T for h in range(kvh)]
    for step in (A3, A1, A2):
        returns[step].wait_recv()
    near = summed([res.at[A0], ra.at[0], ra.at[1], ra.at[2]])
    cross.wait_recv()
    whole = near + rx[...].astype(F32)
    total = jnp.sum(whole[hd:], axis=0, keepdims=True) + own_t[pl.ds(0, 1), :]
    for h in range(kvh):
        lanes = slice(h * half, (h + 1) * half)
        attended = ((whole[:hd, lanes] + own_num[h]) / total[:, lanes]).T.astype(BF16)
        for g in range(half // seqs):
            head = h * (half // seqs) + g
            out_ref[:, pl.ds(head * hd, hd)] = attended[g * seqs : (g + 1) * seqs]

    for copy in gathers.values():
        copy.wait_send()
    for copy in returns.values():
        copy.wait_send()
    cross.wait_send()


def attention(queries, keys, values, hot_pages, hot_used, user_pages, lengths):
    seqs, heads, hd = queries.shape
    pages, kvh, page, _ = keys.shape
    rows = seqs * heads
    half = rows // kvh
    vmem = pltpu.VMEM
    return pl.pallas_call(
        attention_kernel,
        out_shape=jax.ShapeDtypeStruct((seqs, heads * hd), BF16),
        in_specs=[pl.BlockSpec(memory_space=pl.ANY)] * 7,
        out_specs=pl.BlockSpec(memory_space=pltpu.VMEM),
        scratch_shapes=[
            vmem((rows, hd), BF16),
            vmem((1, hot_pages.shape[0]), I32),
            vmem((hot_used.shape[0] // 128, 128), I32),
            vmem((1, seqs), I32),
            pltpu.SMEM((1, seqs), I32),
            vmem((pages, kvh, page, hd), BF16),
            vmem((pages, kvh, page, hd), BF16),
            vmem((2 * HOT_CAP, kvh, page, hd), BF16),
            vmem((2 * HOT_CAP, kvh, page, hd), BF16),
            vmem((kvh, hd, 2 * HOT_CAP * page), BF16),
            vmem((8, hd, rows), BF16),
            vmem((1, kvh * hd, rows), BF16),
            vmem((8, 128), BF16),
            vmem((8, rows), F32),
            vmem((8, rows), F32),
            vmem((2 * HOT_CAP, 128), F32),
            vmem((8, hd + 16, rows), BF16),
            vmem((3, hd + 16, rows), BF16),
            vmem((3, hd + 16, rows), BF16),
            vmem((hd + 16, rows), BF16),
            vmem((hd + 16, rows), BF16),
            vmem((page, rows), F32),
            vmem((rows, page), F32),
            vmem((rows, kvh * hd), F32),
            pltpu.SemaphoreType.DMA((9,)),
            pltpu.SemaphoreType.DMA((2,)),
            pltpu.SemaphoreType.DMA((2,)),
            pltpu.SemaphoreType.DMA((7,)),
            pltpu.SemaphoreType.DMA((7,)),
            pltpu.SemaphoreType.DMA((7,)),
            pltpu.SemaphoreType.DMA((7,)),
        ],
        compiler_params=pltpu.CompilerParams(
            collective_id=0, has_side_effects=True, vmem_limit_bytes=40 * 1024 * 1024
        ),
        name="attention",
    )(
        queries.reshape(rows, hd),
        keys,
        values,
        hot_pages.reshape(1, -1),
        hot_used.reshape(-1, 128),
        user_pages.reshape(1, -1),
        lengths.reshape(1, -1),
    )


def split_up(shard, dim, count):
    shape = shard.shape
    parts = shard.reshape(*shape[:dim], count, shape[dim] // count, *shape[dim + 1 :])
    return jnp.moveaxis(parts, dim, 0)


def sent_and_summed(shard, axis, dim):
    count = lax.axis_size(axis)
    parts = lax.all_to_all(split_up(shard, dim, count), axis, 0, 0, tiled=True)
    return jnp.sum(parts.astype(jnp.float32), axis=0)


def per_device(
    queries, keys, values, hot_pages, hot_used, user_pages, lengths, o_weight, residual, norm_gain
):
    attended = attention(queries, keys, values, hot_pages, hot_used, user_pages, lengths)
    projected = sent_and_summed(
        jnp.dot(attended, o_weight, preferred_element_type=jnp.float32).astype(jnp.bfloat16),
        "heads",
        0,
    )
    mean_sq = jnp.mean(projected * projected, axis=1, keepdims=True)
    normed = projected / jnp.sqrt(mean_sq + epsilon) * norm_gain[None, :]
    return (residual.astype(jnp.float32) + normed).astype(jnp.bfloat16)


def solution(mesh):
    in_specs = (
        P("pages", "heads", None),
        P("pages", "heads", None, None),
        P("pages", "heads", None, None),
        P(),
        P(),
        P("pages", None),
        P("pages"),
        P("heads", None),
        P(("pages", "heads"), None),
        P(),
    )
    out_specs = P(("pages", "heads"), None)
    return jax.shard_map(
        per_device, mesh=mesh, in_specs=in_specs, out_specs=out_specs, check_vma=False
    )
```

```python
import functools
import math

import jax
import jax.numpy as jnp
from jax import lax
from jax.experimental import pallas as pl
from jax.experimental.pallas import tpu as pltpu
from jax.sharding import PartitionSpec as P

HOT_CAP = 8
soft_cap = 50.0
score_scale = 1.0 / 12.0
epsilon = 1e-06
NY = 4
NZ = 4
CHUNKS = 3
F32, BF16, I32 = jnp.float32, jnp.bfloat16, jnp.int32
MESH = pl.DeviceIdType.MESH

A0, A3, A1, A2, B3, B1, B2, B0 = range(8)
OWNER = {A0: (0, 0), A3: (3, 0), A1: (1, 0), A2: (2, 0), B3: (3, 1), B1: (1, 1), B2: (2, 1), B0: (0, 1)}


def weights_of(logits):
    return jnp.exp2(jnp.tanh(logits * (score_scale / soft_cap)) * (soft_cap * math.log2(math.e)))


def split_sum(totals, rows):
    high = totals.astype(BF16).astype(F32)
    row = lax.broadcasted_iota(I32, (16, rows), 0)
    return jnp.where(row == 0, high, jnp.where(row == 1, totals - high, 0.0)).astype(BF16)


def layer_kernel(
    q_hbm, k_hbm, v_hbm, hot_hbm, used_hbm, up_hbm, len_hbm, w_hbm, out_ref,
    q_v, hot_v, used_v, len_v, up_s, kbuf, vbuf, hk, hv, vt, qt, qbd, urow, lrow, pos,
    res, ra, rb, rx, bsum, own_t, own_w, own_o,
    w_v, att, pz, zr, px, xr, near_sum,
    in_sem, z_send, z_recv, x_send, x_recv, kv_send, kv_recv, ag_send, ag_recv, rs_send, rs_recv,
):
    seqs = len_v.shape[1]
    kvh, page, hd = hk.shape[1:]
    rows = q_v.shape[0]
    half = rows // kvh
    me = lax.axis_index("pages")
    y, xh, core = me // 4, (me // 2) % 2, me % 2

    member = lax.axis_index("heads")
    xl, z = member // NZ, member % NZ

    def head_at(dx, dz):
        return {"heads": ((xl + dx) % 2) * NZ + (z + dz) % NZ}

    def seq_at(place):
        return ((place // 8) % 2) * (seqs // 2) + (place // 16) * 8 + place % 8

    def at(dy, dx=0, dc=0):
        return {"pages": ((y + dy) % NY) * 4 + ((xh + dx) % 2) * 2 + (core + dc) % 2}

    def remote(src, dst, send, recv, target):
        return pltpu.make_async_remote_copy(
            src_ref=src, dst_ref=dst, send_sem=send, recv_sem=recv, device_id=target, device_id_type=MESH
        )

    local = [
        pltpu.make_async_copy(q_hbm, q_v, in_sem.at[0]),
        pltpu.make_async_copy(hot_hbm, hot_v, in_sem.at[1]),
        pltpu.make_async_copy(used_hbm, used_v, in_sem.at[2]),
        pltpu.make_async_copy(len_hbm, len_v, in_sem.at[3]),
        pltpu.make_async_copy(up_hbm, up_s, in_sem.at[4]),
        pltpu.make_async_copy(v_hbm.at[pl.ds(0, HOT_CAP)], hv.at[pl.ds(0, HOT_CAP)], in_sem.at[5]),
        pltpu.make_async_copy(k_hbm.at[pl.ds(0, HOT_CAP)], hk.at[pl.ds(0, HOT_CAP)], in_sem.at[6]),
        pltpu.make_async_copy(k_hbm, kbuf, in_sem.at[7]),
        pltpu.make_async_copy(v_hbm, vbuf, in_sem.at[8]),
        pltpu.make_async_copy(w_hbm, w_v, in_sem.at[9]),
    ]
    for copy in local:
        copy.start()

    barrier = pltpu.get_barrier_semaphore()
    peers = [at(1), at(2), at(3), at(0, 1), at(0, 0, 1)]
    peers += [head_at(0, 1), head_at(0, 2), head_at(0, 3), head_at(1, 0)]
    for peer in peers:
        pl.semaphore_signal(barrier, inc=1, device_id=peer, device_id_type=MESH)

    local[0].wait()
    r = lax.broadcasted_iota(I32, (rows, rows), 0)
    col = lax.broadcasted_iota(I32, (rows, rows), 1)
    heads = rows // seqs
    perm = jnp.where(col == seq_at(r % seqs) * heads + r // seqs, 1.0, 0.0).astype(BF16)
    q_rows = jnp.dot(perm, q_v[...], preferred_element_type=F32)
    qt[A0] = q_rows.T.astype(BF16)

    pl.semaphore_wait(barrier, len(peers))

    kv_copies = [
        remote(k_hbm.at[pl.ds(0, HOT_CAP)], hk.at[pl.ds(HOT_CAP, HOT_CAP)], kv_send.at[0], kv_recv.at[0], at(0, 0, 1)),
        remote(v_hbm.at[pl.ds(0, HOT_CAP)], hv.at[pl.ds(HOT_CAP, HOT_CAP)], kv_send.at[1], kv_recv.at[1], at(0, 0, 1)),
    ]
    plan = [(A0, B0, (0, 1)), (A0, A3, (1, 0)), (A0, A1, (3, 0)), (A3, A2, (1, 0)), (B0, B3, (1, 0)), (B0, B1, (3, 0)), (B1, B2, (3, 0))]
    gathers = {
        dst: remote(qt.at[src], qt.at[dst], ag_send.at[k], ag_recv.at[k], at(*to))
        for k, (src, dst, to) in enumerate(plan)
    }
    returns = {}
    for k, step in enumerate((A3, A1, A2, B3, B1, B2)):
        dy, dx = OWNER[step]
        slots = rb if dx else ra
        returns[step] = remote(res.at[step], slots.at[NY - dy - 1], rs_send.at[k], rs_recv.at[k], at(dy))
    cross = remote(bsum, rx, rs_send.at[6], rs_recv.at[6], at(0, 1))

    gathers[B0].start()
    gathers[A3].start()
    gathers[A1].start()
    for copy in kv_copies:
        copy.start()

    for copy in local[1:5]:
        copy.wait()
    lane = lax.broadcasted_iota(I32, (2 * seqs, rows), 0)
    pick = seq_at(lax.broadcasted_iota(I32, (2 * seqs, rows), 1) % seqs)
    spread = jnp.where(lane == core * seqs + pick, 1.0, 0.0).astype(BF16)
    used = jnp.dot(used_v[...].astype(F32).astype(BF16), spread, preferred_element_type=F32)
    own_t[pl.ds(0, 8), :] = used
    for step, (dy, dx) in OWNER.items():
        chip = ((y + dy) % NY) * 2 + (xh + dx) % 2
        urow[pl.ds(step, 1), :] = own_t[pl.ds(chip, 1), :]
    lane = lax.broadcasted_iota(I32, (seqs, rows), 0)
    pick = seq_at(lax.broadcasted_iota(I32, (seqs, rows), 1) % seqs)
    spread = jnp.where(lane == pick, 1.0, 0.0).astype(BF16)
    lens = jnp.broadcast_to(len_v[...].astype(F32), (8, seqs)).astype(BF16)
    lrow[...] = jnp.dot(lens, spread, preferred_element_type=F32)
    hot_n = hot_v.shape[1]
    cand = lax.broadcasted_iota(I32, (2 * HOT_CAP, hot_n), 0)
    group = jnp.where(cand < HOT_CAP, me, at(0, 0, 1)["pages"])
    match = hot_v[...] == group * k_hbm.shape[0] + cand % HOT_CAP
    order = lax.broadcasted_iota(I32, (2 * HOT_CAP, hot_n), 1).astype(F32)
    pos[...] = jnp.broadcast_to(
        jnp.min(jnp.where(match, order, 1e9), axis=1, keepdims=True), pos.shape
    )

    qbd[...] = jnp.zeros_like(qbd)

    def set_queries(step):
        qbd[0, pl.ds(0, hd), pl.ds(0, half)] = qt[step, :, pl.ds(0, half)]
        qbd[0, pl.ds(hd, hd), pl.ds(half, half)] = qt[step, :, pl.ds(half, half)]

    def transpose_values(first):
        for j in range(first, first + HOT_CAP):
            for h in range(kvh):
                vt[h, :, pl.ds(j * page, page)] = hv[j, h].T

    local[5].wait()
    transpose_values(0)
    local[6].wait()

    def shared_block(step):
        set_queries(step)
        allowed = jnp.where(urow[pl.ds(step, 1), :] > pos[:, pl.ds(0, 1)], 1.0, 0.0)
        total = jnp.zeros((1, rows), F32)
        parts = [jnp.zeros((hd, half), F32) for _ in range(kvh)]
        for c in range(HOT_CAP):
            keys = jnp.concatenate(
                [hk[pl.ds(2 * c, 2), h].reshape(2 * page, hd) for h in range(kvh)], axis=1
            )
            logits = jnp.dot(keys, qbd[0], preferred_element_type=F32)
            weight = weights_of(logits)
            weight = jnp.concatenate(
                [weight[i * page : (i + 1) * page] * allowed[2 * c + i : 2 * c + i + 1] for i in range(2)], axis=0
            )
            total = total + jnp.sum(weight, axis=0, keepdims=True)
            rounded = weight.astype(BF16)
            for h in range(kvh):
                parts[h] = parts[h] + jnp.dot(
                    vt[h, :, pl.ds(2 * c * page, 2 * page)],
                    rounded[:, h * half : (h + 1) * half],
                    preferred_element_type=F32,
                )
        for h in range(kvh):
            res[step, pl.ds(0, hd), pl.ds(h * half, half)] = parts[h].astype(BF16)
        res[step, pl.ds(hd, 16), :] = split_sum(total, rows)

    def own_scores():
        local[7].wait()
        set_queries(A0)

        def four(g, carry):
            seq_of = lax.broadcasted_iota(I32, (page, rows), 1) % seqs
            tile = own_t[...]
            for i in range(0, 4, 2):
                pages = [up_s[0, seq_at(g * 4 + i + j)] for j in range(2)]
                keys = jnp.concatenate(
                    [jnp.concatenate([kbuf[u, h] for h in range(kvh)], axis=1) for u in pages], axis=0
                )
                logits = jnp.dot(keys, qbd[0], preferred_element_type=F32)
                for j in range(2):
                    tile = jnp.where(seq_of == g * 4 + i + j, logits[j * page : (j + 1) * page], tile)
            own_t[...] = tile
            return carry

        own_t[...] = jnp.zeros_like(own_t)
        lax.fori_loop(0, seqs // 4, four, 0)
        token = lax.broadcasted_iota(I32, (page, rows), 0).astype(F32)
        weight = jnp.where(token < lrow[pl.ds(0, 1), :], weights_of(own_t[...]), 0.0)
        own_t[pl.ds(0, 8), :] = jnp.broadcast_to(jnp.sum(weight, axis=0, keepdims=True), (8, rows))
        own_w[...] = weight.T

    def own_values():
        local[8].wait()
        own_o[...] = jnp.zeros_like(own_o)

        def eight(g, carry):
            seq_of = lax.broadcasted_iota(I32, (rows, page), 0) % seqs
            left, right = [], []
            for i in range(8):
                u = up_s[0, seq_at(g * 8 + i)]
                left.append(jnp.where(seq_of == g * 8 + i, own_w[...], 0.0).astype(BF16))
                right.append(jnp.concatenate([vbuf[u, h] for h in range(kvh)], axis=1))
            own_o[...] += jnp.dot(
                jnp.concatenate(left, axis=1), jnp.concatenate(right, axis=0), preferred_element_type=F32
            )
            return carry

        lax.fori_loop(0, seqs // 8, eight, 0)

    own_scores()
    kv_copies[0].wait()
    kv_copies[1].wait()
    transpose_values(HOT_CAP)

    def one_step(step, carry):
        for k in (A3, A1, A2, B3, B1, B2):
            @pl.when(step == k)
            def _():
                gathers[k].wait_recv()

        @pl.when(step == A3)
        def _():
            gathers[A2].start()

        @pl.when(step == A1)
        def _():
            gathers[B0].wait_recv()
            gathers[B3].start()
            gathers[B1].start()

        @pl.when(step == B1)
        def _():
            gathers[B2].start()

        shared_block(step)
        for k in (A3, A1, A2, B3, B1, B2):
            @pl.when(step == k)
            def _():
                returns[k].start()
        return carry

    lax.fori_loop(0, 8, one_step, 0)
    own_values()

    def summed(pieces):
        return sum(piece[...].astype(F32) for piece in pieces)

    for step in (B3, B1, B2):
        returns[step].wait_recv()
    whole = summed([res.at[B0], rb.at[0], rb.at[1], rb.at[2]])
    bsum[pl.ds(0, hd), :] = whole[:hd].astype(BF16)
    bsum[pl.ds(hd, 16), :] = split_sum(jnp.sum(whole[hd:], axis=0, keepdims=True), rows)
    cross.start()
    own_num = [own_o[pl.ds(h * half, half), pl.ds(h * hd, hd)].T for h in range(kvh)]
    for step in (A3, A1, A2):
        returns[step].wait_recv()
    near = summed([res.at[A0], ra.at[0], ra.at[1], ra.at[2]])
    cross.wait_recv()
    whole = near + rx[...].astype(F32)
    total = jnp.sum(whole[hd:], axis=0, keepdims=True) + own_t[pl.ds(0, 1), :]
    for h in range(kvh):
        lanes = slice(h * half, (h + 1) * half)
        attended = ((whole[:hd, lanes] + own_num[h]) / total[:, lanes]).T.astype(BF16)
        for g in range(half // seqs):
            head = h * (half // seqs) + g
            att[:, pl.ds(head * hd, hd)] = attended[g * seqs : (g + 1) * seqs]

    local[9].wait()
    block = seqs // NZ
    width = w_v.shape[1] // CHUNKS
    to_z, to_x = [], []
    for k in range(CHUNKS):
        cols = pl.ds(k * width, width)
        piece = jnp.dot(att[...], w_v[:, cols], preferred_element_type=F32).astype(BF16)
        for i in range(NZ):
            pz[i, :, cols] = piece[i * block : (i + 1) * block]
        copies = []
        for d in (1, 3, 2):
            n = k * 3 + d - 1
            copies.append(
                remote(pz.at[(z + d) % NZ, :, cols], zr.at[NZ - d - 1, :, cols], z_send.at[n], z_recv.at[n], head_at(0, d))
            )
            copies[-1].start()
        to_z.append(copies)
    for k in range(CHUNKS):
        cols = pl.ds(k * width, width)
        for copy in to_z[k]:
            copy.wait_recv()
        both = pz[z, :, cols].astype(F32)
        for i in range(NZ - 1):
            both = both + zr[i, :, cols].astype(F32)
        first, second = both[: block // 2], both[block // 2 :]
        near_sum[:, cols] = jnp.where(xl == 0, first, second)
        px[:, cols] = jnp.where(xl == 0, second, first).astype(BF16)
        copy = remote(px.at[:, cols], xr.at[:, cols], x_send.at[k], x_recv.at[k], head_at(1, 0))
        copy.start()
        to_x.append(copy)
    square = jnp.zeros((block // 2, 1), F32)
    for k in range(CHUNKS):
        cols = pl.ds(k * width, width)
        to_x[k].wait_recv()
        projected = near_sum[:, cols] + xr[:, cols].astype(F32)
        near_sum[:, cols] = projected
        square = square + jnp.sum(projected * projected, axis=1, keepdims=True)
    out_ref[...] = near_sum[...] / jnp.sqrt(square / w_v.shape[1] + epsilon)

    for copy in (*gathers.values(), *returns.values(), cross, *sum(to_z, []), *to_x):
        copy.wait_send()


def layer(queries, keys, values, hot_pages, hot_used, user_pages, lengths, o_weight):
    seqs, heads, hd = queries.shape
    pages, kvh, page, _ = keys.shape
    rows = seqs * heads
    width = o_weight.shape[1]
    vmem = pltpu.VMEM
    return pl.pallas_call(
        layer_kernel,
        out_shape=jax.ShapeDtypeStruct((seqs // 8, width), F32),
        in_specs=[pl.BlockSpec(memory_space=pl.ANY)] * 8,
        out_specs=pl.BlockSpec(memory_space=pltpu.VMEM),
        scratch_shapes=[
            vmem((rows, hd), BF16),
            vmem((1, hot_pages.shape[0]), I32),
            vmem((hot_used.shape[0] // 128, 128), I32),
            vmem((1, seqs), I32),
            pltpu.SMEM((1, seqs), I32),
            vmem((pages, kvh, page, hd), BF16),
            vmem((pages, kvh, page, hd), BF16),
            vmem((2 * HOT_CAP, kvh, page, hd), BF16),
            vmem((2 * HOT_CAP, kvh, page, hd), BF16),
            vmem((kvh, hd, 2 * HOT_CAP * page), BF16),
            vmem((8, hd, rows), BF16),
            vmem((1, kvh * hd, rows), BF16),
            vmem((8, rows), F32),
            vmem((8, rows), F32),
            vmem((2 * HOT_CAP, 128), F32),
            vmem((8, hd + 16, rows), BF16),
            vmem((3, hd + 16, rows), BF16),
            vmem((3, hd + 16, rows), BF16),
            vmem((hd + 16, rows), BF16),
            vmem((hd + 16, rows), BF16),
            vmem((page, rows), F32),
            vmem((rows, page), F32),
            vmem((rows, kvh * hd), F32),
            vmem(o_weight.shape, BF16),
            vmem((seqs, heads * hd), BF16),
            vmem((NZ, seqs // NZ, width), BF16),
            vmem((NZ - 1, seqs // NZ, width), BF16),
            vmem((seqs // 8, width), BF16),
            vmem((seqs // 8, width), BF16),
            vmem((seqs // 8, width), F32),
            pltpu.SemaphoreType.DMA((10,)),
            pltpu.SemaphoreType.DMA((3 * CHUNKS,)),
            pltpu.SemaphoreType.DMA((3 * CHUNKS,)),
            pltpu.SemaphoreType.DMA((CHUNKS,)),
            pltpu.SemaphoreType.DMA((CHUNKS,)),
            pltpu.SemaphoreType.DMA((2,)),
            pltpu.SemaphoreType.DMA((2,)),
            pltpu.SemaphoreType.DMA((7,)),
            pltpu.SemaphoreType.DMA((7,)),
            pltpu.SemaphoreType.DMA((7,)),
            pltpu.SemaphoreType.DMA((7,)),
        ],
        compiler_params=pltpu.CompilerParams(
            collective_id=0, has_side_effects=True, vmem_limit_bytes=66_000_000
        ),
        name="layer",
    )(
        queries.reshape(rows, hd),
        keys,
        values,
        hot_pages.reshape(1, -1),
        hot_used.reshape(-1, 128),
        user_pages.reshape(1, -1),
        lengths.reshape(1, -1),
        o_weight,
    )


def per_device(
    queries, keys, values, hot_pages, hot_used, user_pages, lengths, o_weight, residual, norm_gain
):
    normed = layer(queries, keys, values, hot_pages, hot_used, user_pages, lengths, o_weight)
    return (residual.astype(F32) + normed * norm_gain[None, :]).astype(BF16)


def solution(mesh):
    in_specs = (
        P("pages", "heads", None),
        P("pages", "heads", None, None),
        P("pages", "heads", None, None),
        P(),
        P(),
        P("pages", None),
        P("pages"),
        P("heads", None),
        P(("pages", "heads"), None),
        P(),
    )
    out_specs = P(("pages", "heads"), None)
    return jax.shard_map(
        per_device, mesh=mesh, in_specs=in_specs, out_specs=out_specs, check_vma=False
    )
```

```python
import functools
import math

import jax
import jax.numpy as jnp
from jax import lax
from jax.experimental import pallas as pl
from jax.experimental.pallas import tpu as pltpu
from jax.sharding import PartitionSpec as P

HOT_CAP = 8
soft_cap = 50.0
score_scale = 1.0 / 12.0
epsilon = 1e-06
NY = 4
NZ = 4
CHUNKS = 4
F32, BF16, I32 = jnp.float32, jnp.bfloat16, jnp.int32
MESH = pl.DeviceIdType.MESH

A3, A1, A2, B0, B3, B1, B2, A0 = range(8)
OWNER = {A3: (3, 0), A1: (1, 0), A2: (2, 0), B0: (0, 1), B3: (3, 1), B1: (1, 1), B2: (2, 1), A0: (0, 0)}


def weights_of(logits):
    return jnp.exp2(jnp.tanh(logits * (score_scale / soft_cap)) * (soft_cap * math.log2(math.e)))


def split_sum(totals, rows):
    high = totals.astype(BF16).astype(F32)
    row = lax.broadcasted_iota(I32, (16, rows), 0)
    return jnp.where(row == 0, high, jnp.where(row == 1, totals - high, 0.0)).astype(BF16)


def layer_kernel(
    q_hbm, k_hbm, v_hbm, hot_hbm, used_hbm, up_hbm, len_hbm, w_hbm, out_ref,
    q_v, hot_v, used_v, len_v, up_s, kbuf, vbuf, hk, hv, vt, qt, qbd, urow, lrow, pos,
    res, ra, own_t, own_w, own_o,
    w_v, att, pz, zt, zj, zr, px, xr, near_sum,
    in_sem, z_send, z_recv, x_send, x_recv, kv_send, kv_recv, ag_send, ag_recv, rs_send, rs_recv, far_sem,
):
    seqs = len_v.shape[1]
    kvh, page, hd = hk.shape[1:]
    rows = q_v.shape[0]
    half = rows // kvh
    me = lax.axis_index("pages")
    y, xh, core = me // 4, (me // 2) % 2, me % 2

    member = lax.axis_index("heads")
    xl, z = member // NZ, member % NZ

    def head_at(dx, dz):
        return {"heads": ((xl + dx) % 2) * NZ + (z + dz) % NZ}

    def seq_at(place):
        return ((place // 8) % 2) * (seqs // 2) + (place // 16) * 8 + place % 8

    def at(dy, dx=0, dc=0):
        return {"pages": ((y + dy) % NY) * 4 + ((xh + dx) % 2) * 2 + (core + dc) % 2}

    def remote(src, dst, send, recv, target):
        return pltpu.make_async_remote_copy(
            src_ref=src, dst_ref=dst, send_sem=send, recv_sem=recv, device_id=target, device_id_type=MESH
        )

    own = pl.ds(HOT_CAP, k_hbm.shape[0] - HOT_CAP)
    hot = pl.ds(0, HOT_CAP)
    local = [
        pltpu.make_async_copy(q_hbm, q_v, in_sem.at[0]),
        pltpu.make_async_copy(hot_hbm, hot_v, in_sem.at[1]),
        pltpu.make_async_copy(used_hbm, used_v, in_sem.at[2]),
        pltpu.make_async_copy(len_hbm, len_v, in_sem.at[3]),
        pltpu.make_async_copy(up_hbm, up_s, in_sem.at[4]),
        pltpu.make_async_copy(k_hbm.at[hot], hk.at[hot], in_sem.at[5]),
        pltpu.make_async_copy(v_hbm.at[hot], hv.at[hot], in_sem.at[6]),
        pltpu.make_async_copy(k_hbm.at[own], kbuf, in_sem.at[7]),
        pltpu.make_async_copy(v_hbm.at[own], vbuf, in_sem.at[8]),
        pltpu.make_async_copy(w_hbm, w_v, in_sem.at[9]),
    ]
    for copy in local[:8]:
        copy.start()

    barrier = pltpu.get_barrier_semaphore()
    peers = [at(1), at(2), at(3), at(0, 1), at(0, 0, 1)]
    peers += [head_at(0, 1), head_at(0, 2), head_at(0, 3), head_at(1, 0)]
    for peer in peers:
        pl.semaphore_signal(barrier, inc=1, device_id=peer, device_id_type=MESH)

    local[0].wait()
    r = lax.broadcasted_iota(I32, (rows, rows), 0)
    col = lax.broadcasted_iota(I32, (rows, rows), 1)
    heads = rows // seqs
    perm = jnp.where(col == seq_at(r % seqs) * heads + r // seqs, 1.0, 0.0).astype(BF16)
    q_rows = jnp.dot(perm, q_v[...], preferred_element_type=F32)
    qt[A0] = q_rows.T.astype(BF16)

    pl.semaphore_wait(barrier, len(peers))

    far = pl.ds(HOT_CAP, HOT_CAP)
    kv_copies = [
        remote(hk.at[hot], hk.at[far], kv_send.at[0], kv_recv.at[0], at(0, 0, 1)),
        remote(hv.at[hot], hv.at[far], kv_send.at[1], kv_recv.at[1], at(0, 0, 1)),
    ]
    gathers, returns = {}, {}
    for step, (dy, dx) in OWNER.items():
        if step == A0:
            continue
        back = next(k for k, at_ in OWNER.items() if at_ == ((NY - dy) % NY, dx))
        gathers[step] = remote(qt.at[A0], qt.at[step], ag_send.at[step], ag_recv.at[step], at((NY - dy) % NY, dx))
        returns[step] = remote(res.at[step], ra.at[back], rs_send.at[step], rs_recv.at[back], at(dy, dx))
    arrivals = {
        step: remote(res.at[step], ra.at[step], rs_send.at[step], rs_recv.at[step], at(0, 1)) for step in returns
    }

    pl.semaphore_signal(far_sem, inc=1, device_id=at(0, 1), device_id_type=MESH)
    for step in (A3, A1, A2, B0):
        gathers[step].start()
    local[5].wait()
    local[6].wait()
    for copy in kv_copies:
        copy.start()
    local[8].start()
    local[9].start()

    for copy in local[1:5]:
        copy.wait()
    lane = lax.broadcasted_iota(I32, (2 * seqs, rows), 0)
    pick = seq_at(lax.broadcasted_iota(I32, (2 * seqs, rows), 1) % seqs)
    spread = jnp.where(lane == core * seqs + pick, 1.0, 0.0).astype(BF16)
    used = jnp.dot(used_v[...].astype(F32).astype(BF16), spread, preferred_element_type=F32)
    own_t[pl.ds(0, 8), :] = used
    for step, (dy, dx) in OWNER.items():
        chip = ((y + dy) % NY) * 2 + (xh + dx) % 2
        urow[pl.ds(step, 1), :] = own_t[pl.ds(chip, 1), :]
    lane = lax.broadcasted_iota(I32, (seqs, rows), 0)
    pick = seq_at(lax.broadcasted_iota(I32, (seqs, rows), 1) % seqs)
    spread = jnp.where(lane == pick, 1.0, 0.0).astype(BF16)
    lens = jnp.broadcast_to(len_v[...].astype(F32), (8, seqs)).astype(BF16)
    lrow[...] = jnp.dot(lens, spread, preferred_element_type=F32)
    hot_n = hot_v.shape[1]
    cand = lax.broadcasted_iota(I32, (2 * HOT_CAP, hot_n), 0)
    group = jnp.where(cand < HOT_CAP, me, at(0, 0, 1)["pages"])
    match = hot_v[...] == group * k_hbm.shape[0] + cand % HOT_CAP
    order = lax.broadcasted_iota(I32, (2 * HOT_CAP, hot_n), 1).astype(F32)
    pos[...] = jnp.broadcast_to(
        jnp.min(jnp.where(match, order, 1e9), axis=1, keepdims=True), pos.shape
    )

    qbd[...] = jnp.zeros_like(qbd)

    def set_queries(step):
        qbd[0, pl.ds(0, hd), pl.ds(0, half)] = qt[step, :, pl.ds(0, half)]
        qbd[0, pl.ds(hd, hd), pl.ds(half, half)] = qt[step, :, pl.ds(half, half)]

    def transpose_values(first):
        for j in range(first, first + HOT_CAP):
            for h in range(kvh):
                vt[h, :, pl.ds(j * page, page)] = hv[j, h].T

    transpose_values(0)

    def shared_block(step):
        set_queries(step)
        allowed = jnp.where(urow[pl.ds(step, 1), :] > pos[:, pl.ds(0, 1)], 1.0, 0.0)
        total = jnp.zeros((1, rows), F32)
        parts = [jnp.zeros((hd, half), F32) for _ in range(kvh)]
        for c in range(HOT_CAP):
            keys = jnp.concatenate(
                [hk[pl.ds(2 * c, 2), h].reshape(2 * page, hd) for h in range(kvh)], axis=1
            )
            logits = jnp.dot(keys, qbd[0], preferred_element_type=F32)
            weight = weights_of(logits)
            weight = jnp.concatenate(
                [weight[i * page : (i + 1) * page] * allowed[2 * c + i : 2 * c + i + 1] for i in range(2)], axis=0
            )
            total = total + jnp.sum(weight, axis=0, keepdims=True)
            rounded = weight.astype(BF16)
            for h in range(kvh):
                parts[h] = parts[h] + jnp.dot(
                    vt[h, :, pl.ds(2 * c * page, 2 * page)],
                    rounded[:, h * half : (h + 1) * half],
                    preferred_element_type=F32,
                )
        for h in range(kvh):
            res[step, pl.ds(0, hd), pl.ds(h * half, half)] = parts[h].astype(BF16)
        res[step, pl.ds(hd, 16), :] = split_sum(total, rows)

    def page_of(place):
        return jnp.maximum(up_s[0, seq_at(place)] - HOT_CAP, 0)

    def own_scores():
        local[7].wait()
        set_queries(A0)

        def some(g, carry):
            seq_of = lax.broadcasted_iota(I32, (page, rows), 1) % seqs
            tile = own_t[...]
            for i in range(0, 16, 2):
                pages = [page_of(g * 16 + i + j) for j in range(2)]
                keys = jnp.concatenate(
                    [jnp.concatenate([kbuf[u, h] for h in range(kvh)], axis=1) for u in pages], axis=0
                )
                logits = jnp.dot(keys, qbd[0], preferred_element_type=F32)
                for j in range(2):
                    tile = jnp.where(seq_of == g * 16 + i + j, logits[j * page : (j + 1) * page], tile)
            own_t[...] = tile
            return carry

        own_t[...] = jnp.zeros_like(own_t)
        lax.fori_loop(0, seqs // 16, some, 0)

    def own_weights():
        token = lax.broadcasted_iota(I32, (page, rows), 0).astype(F32)
        weight = jnp.where(token < lrow[pl.ds(0, 1), :], weights_of(own_t[...]), 0.0)
        own_t[pl.ds(0, 8), :] = jnp.broadcast_to(jnp.sum(weight, axis=0, keepdims=True), (8, rows))
        own_w[...] = weight.T

    def own_values():
        local[8].wait()

        def some(n, carry):
            row = lax.broadcasted_iota(I32, (8 * heads, page), 0) % 8
            for m in range(4):
                g = n * 4 + m
                weight = jnp.concatenate([own_w[pl.ds(h * seqs + g * 8, 8), :] for h in range(heads)], axis=0)
                left, right = [], []
                for i in range(8):
                    u = page_of(g * 8 + i)
                    left.append(jnp.where(row == i, weight, 0.0).astype(BF16))
                    right.append(jnp.concatenate([vbuf[u, h] for h in range(kvh)], axis=1))
                part = jnp.dot(
                    jnp.concatenate(left, axis=1), jnp.concatenate(right, axis=0), preferred_element_type=F32
                )
                for h in range(heads):
                    own_o[pl.ds(h * seqs + g * 8, 8), :] = part[h * 8 : (h + 1) * 8]
            return carry

        lax.fori_loop(0, seqs // 32, some, 0)

    own_scores()
    pl.semaphore_wait(far_sem, 1)
    for step in (B3, B1, B2):
        gathers[step].start()
    own_weights()
    kv_copies[0].wait()
    kv_copies[1].wait()
    transpose_values(HOT_CAP)

    def one_step(step, carry):
        for k in gathers:
            @pl.when(step == k)
            def _():
                gathers[k].wait_recv()

        shared_block(step)
        for k in returns:
            @pl.when(step == k)
            def _():
                returns[k].start()
        return carry

    lax.fori_loop(0, 8, one_step, 0)
    own_values()

    def summed(pieces):
        return sum(piece[...].astype(F32) for piece in pieces)

    own_num = [own_o[pl.ds(h * half, half), pl.ds(h * hd, hd)].T for h in range(kvh)]
    for copy in arrivals.values():
        copy.wait_recv()
    whole = summed([res.at[A0], *(ra.at[k] for k in arrivals)])
    total = jnp.sum(whole[hd:], axis=0, keepdims=True) + own_t[pl.ds(0, 1), :]
    for h in range(kvh):
        lanes = slice(h * half, (h + 1) * half)
        attended = ((whole[:hd, lanes] + own_num[h]) / total[:, lanes]).T.astype(BF16)
        for g in range(half // seqs):
            head = h * (half // seqs) + g
            att[:, pl.ds(head * hd, hd)] = attended[g * seqs : (g + 1) * seqs]

    local[9].wait()
    block = seqs // NZ
    width = w_v.shape[1] // CHUNKS
    relayed, plain, joined, to_x = {}, {}, {}, {}
    order = [k // 2 + (k % 2) * (CHUNKS // 2) for k in range(CHUNKS)]
    for k in order:
        via, other = (1, 3) if k < CHUNKS // 2 else (3, 1)
        cols = pl.ds(k * width, width)
        piece = jnp.dot(att[...], w_v[:, cols], preferred_element_type=F32).astype(BF16)
        for i in range(NZ):
            pz[i, :, cols] = piece[i * block : (i + 1) * block]
        relayed[k] = remote(
            pz.at[(z + 2) % NZ, :, cols], zt.at[:, cols], z_send.at[k], z_recv.at[k], head_at(0, via)
        )
        plain[k] = remote(
            pz.at[(z + other) % NZ, :, cols], zr.at[other // 2, :, cols],
            z_send.at[CHUNKS + k], z_recv.at[CHUNKS + k], head_at(0, other),
        )
        joined[k] = remote(
            zj.at[:, cols], zr.at[via // 2, :, cols],
            z_send.at[2 * CHUNKS + k], z_recv.at[2 * CHUNKS + k], head_at(0, via),
        )
        relayed[k].start()
        plain[k].start()
    for k in order:
        via = 1 if k < CHUNKS // 2 else 3
        cols = pl.ds(k * width, width)
        relayed[k].wait_recv()
        zj[:, cols] = (pz[(z + via) % NZ, :, cols].astype(F32) + zt[:, cols].astype(F32)).astype(BF16)
        joined[k].start()
    for k in order:
        cols = pl.ds(k * width, width)
        plain[k].wait_recv()
        joined[k].wait_recv()
        both = pz[z, :, cols].astype(F32) + zr[0, :, cols].astype(F32) + zr[1, :, cols].astype(F32)
        first, second = both[: block // 2], both[block // 2 :]
        near_sum[:, cols] = jnp.where(xl == 0, first, second)
        px[:, cols] = jnp.where(xl == 0, second, first).astype(BF16)
        to_x[k] = remote(px.at[:, cols], xr.at[:, cols], x_send.at[k], x_recv.at[k], head_at(1, 0))
        to_x[k].start()
    square = jnp.zeros((block // 2, 1), F32)
    for k in order:
        cols = pl.ds(k * width, width)
        to_x[k].wait_recv()
        projected = near_sum[:, cols] + xr[:, cols].astype(F32)
        near_sum[:, cols] = projected
        square = square + jnp.sum(projected * projected, axis=1, keepdims=True)
    out_ref[...] = near_sum[...] / jnp.sqrt(square / w_v.shape[1] + epsilon)

    for copy in (*gathers.values(), *returns.values(), *relayed.values(), *plain.values(), *joined.values(), *to_x.values()):
        copy.wait_send()


def layer(queries, keys, values, hot_pages, hot_used, user_pages, lengths, o_weight):
    seqs, heads, hd = queries.shape
    pages, kvh, page, _ = keys.shape
    rows = seqs * heads
    width = o_weight.shape[1]
    vmem = pltpu.VMEM
    return pl.pallas_call(
        layer_kernel,
        out_shape=jax.ShapeDtypeStruct((seqs // 8, width), F32),
        in_specs=[pl.BlockSpec(memory_space=pl.ANY)] * 8,
        out_specs=pl.BlockSpec(memory_space=pltpu.VMEM),
        scratch_shapes=[
            vmem((rows, hd), BF16),
            vmem((1, hot_pages.shape[0]), I32),
            vmem((hot_used.shape[0] // 128, 128), I32),
            vmem((1, seqs), I32),
            pltpu.SMEM((1, seqs), I32),
            vmem((pages - HOT_CAP, kvh, page, hd), BF16),
            vmem((pages - HOT_CAP, kvh, page, hd), BF16),
            vmem((2 * HOT_CAP, kvh, page, hd), BF16),
            vmem((2 * HOT_CAP, kvh, page, hd), BF16),
            vmem((kvh, hd, 2 * HOT_CAP * page), BF16),
            vmem((8, hd, rows), BF16),
            vmem((1, kvh * hd, rows), BF16),
            vmem((8, rows), F32),
            vmem((8, rows), F32),
            vmem((2 * HOT_CAP, 128), F32),
            vmem((8, hd + 16, rows), BF16),
            vmem((7, hd + 16, rows), BF16),
            vmem((page, rows), F32),
            vmem((rows, page), F32),
            vmem((rows, kvh * hd), F32),
            vmem(o_weight.shape, BF16),
            vmem((seqs, heads * hd), BF16),
            vmem((NZ, seqs // NZ, width), BF16),
            vmem((seqs // NZ, width), BF16),
            vmem((seqs // NZ, width), BF16),
            vmem((2, seqs // NZ, width), BF16),
            vmem((seqs // 8, width), BF16),
            vmem((seqs // 8, width), BF16),
            vmem((seqs // 8, width), F32),
            pltpu.SemaphoreType.DMA((10,)),
            pltpu.SemaphoreType.DMA((3 * CHUNKS,)),
            pltpu.SemaphoreType.DMA((3 * CHUNKS,)),
            pltpu.SemaphoreType.DMA((CHUNKS,)),
            pltpu.SemaphoreType.DMA((CHUNKS,)),
            pltpu.SemaphoreType.DMA((2,)),
            pltpu.SemaphoreType.DMA((2,)),
            pltpu.SemaphoreType.DMA((7,)),
            pltpu.SemaphoreType.DMA((7,)),
            pltpu.SemaphoreType.DMA((7,)),
            pltpu.SemaphoreType.DMA((7,)),
            pltpu.SemaphoreType.REGULAR,
        ],
        compiler_params=pltpu.CompilerParams(
            collective_id=0, has_side_effects=True, vmem_limit_bytes=66_000_000
        ),
        name="layer",
    )(
        queries.reshape(rows, hd),
        keys,
        values,
        hot_pages.reshape(1, -1),
        hot_used.reshape(-1, 128),
        user_pages.reshape(1, -1),
        lengths.reshape(1, -1),
        o_weight,
    )


def per_device(
    queries, keys, values, hot_pages, hot_used, user_pages, lengths, o_weight, residual, norm_gain
):
    normed = layer(queries, keys, values, hot_pages, hot_used, user_pages, lengths, o_weight)
    return (residual.astype(F32) + normed * norm_gain[None, :]).astype(BF16)


def solution(mesh):
    in_specs = (
        P("pages", "heads", None),
        P("pages", "heads", None, None),
        P("pages", "heads", None, None),
        P(),
        P(),
        P("pages", None),
        P("pages"),
        P("heads", None),
        P(("pages", "heads"), None),
        P(),
    )
    out_specs = P(("pages", "heads"), None)
    return jax.shard_map(
        per_device, mesh=mesh, in_specs=in_specs, out_specs=out_specs, check_vma=False
    )
```

```python
import functools
import math

import jax
import jax.numpy as jnp
from jax import lax
from jax.experimental import pallas as pl
from jax.experimental.pallas import tpu as pltpu
from jax.sharding import PartitionSpec as P

HOT_CAP = 8
soft_cap = 50.0
score_scale = 1.0 / 12.0
epsilon = 1e-06
NY = 4
NZ = 4
CHUNKS = 4
F32, BF16, I32 = jnp.float32, jnp.bfloat16, jnp.int32
MESH = pl.DeviceIdType.MESH

A3, B0, A1, B3, B1, B2, A2, A0 = range(8)
OWNER = {A3: (3, 0), A1: (1, 0), A2: (2, 0), B0: (0, 1), B3: (3, 1), B1: (1, 1), B2: (2, 1), A0: (0, 0)}


def weights_of(logits):
    return jnp.exp2(jnp.tanh(logits * (score_scale / soft_cap)) * (soft_cap * math.log2(math.e)))


def split_sum(totals, rows):
    high = totals.astype(BF16).astype(F32)
    row = lax.broadcasted_iota(I32, (16, rows), 0)
    return jnp.where(row == 0, high, jnp.where(row == 1, totals - high, 0.0)).astype(BF16)


def layer_kernel(
    q_hbm, k_hbm, v_hbm, hot_hbm, used_hbm, up_hbm, len_hbm, w_hbm, out_ref,
    q_v, hot_v, used_v, len_v, up_s, kbuf, vbuf, hk, hv, vt, qt, qbd, urow, lrow, pos,
    wt, res, ra, own_t, own_w, own_o,
    w_v, att, pz, zt, zj, zr, near_sum,
    in_sem, z_send, z_recv, kv_send, kv_recv, ag_send, ag_recv, rs_send, rs_recv, far_sem,
):
    seqs = len_v.shape[1]
    kvh, page, hd = hk.shape[1:]
    rows = q_v.shape[0]
    half = rows // kvh
    me = lax.axis_index("pages")
    y, xh, core = me // 4, (me // 2) % 2, me % 2

    member = lax.axis_index("heads")
    xl, z = member // NZ, member % NZ

    def head_at(dx, dz):
        return {"heads": ((xl + dx) % 2) * NZ + (z + dz) % NZ}

    def seq_at(place):
        return ((place // 8) % 2) * (seqs // 2) + (place // 16) * 8 + place % 8

    def at(dy, dx=0, dc=0):
        return {"pages": ((y + dy) % NY) * 4 + ((xh + dx) % 2) * 2 + (core + dc) % 2}

    def remote(src, dst, send, recv, target):
        return pltpu.make_async_remote_copy(
            src_ref=src, dst_ref=dst, send_sem=send, recv_sem=recv, device_id=target, device_id_type=MESH
        )

    own = pl.ds(HOT_CAP, k_hbm.shape[0] - HOT_CAP)
    hot = pl.ds(0, HOT_CAP)
    local = [
        pltpu.make_async_copy(q_hbm, q_v, in_sem.at[0]),
        pltpu.make_async_copy(hot_hbm, hot_v, in_sem.at[1]),
        pltpu.make_async_copy(used_hbm, used_v, in_sem.at[2]),
        pltpu.make_async_copy(len_hbm, len_v, in_sem.at[3]),
        pltpu.make_async_copy(up_hbm, up_s, in_sem.at[4]),
        pltpu.make_async_copy(k_hbm.at[hot], hk.at[hot], in_sem.at[5]),
        pltpu.make_async_copy(v_hbm.at[hot], hv.at[hot], in_sem.at[6]),
        pltpu.make_async_copy(k_hbm.at[own], kbuf, in_sem.at[7]),
        pltpu.make_async_copy(v_hbm.at[own], vbuf, in_sem.at[8]),
        pltpu.make_async_copy(w_hbm, w_v, in_sem.at[9]),
    ]
    for copy in local[:8]:
        copy.start()

    barrier = pltpu.get_barrier_semaphore()
    peers = [at(1), at(2), at(3), at(0, 1), at(0, 0, 1)]
    peers += [head_at(0, 1), head_at(0, 2), head_at(0, 3), head_at(1, 0)]
    for peer in peers:
        pl.semaphore_signal(barrier, inc=1, device_id=peer, device_id_type=MESH)

    local[0].wait()
    r = lax.broadcasted_iota(I32, (rows, rows), 0)
    col = lax.broadcasted_iota(I32, (rows, rows), 1)
    heads = rows // seqs
    perm = jnp.where(col == seq_at(r % seqs) * heads + r // seqs, 1.0, 0.0).astype(BF16)
    q_rows = jnp.dot(perm, q_v[...], preferred_element_type=F32)
    qt[A0] = q_rows.T.astype(BF16)

    pl.semaphore_wait(barrier, len(peers))

    far = pl.ds(HOT_CAP, HOT_CAP)
    kv_copies = [
        remote(hk.at[hot], hk.at[far], kv_send.at[0], kv_recv.at[0], at(0, 0, 1)),
        remote(hv.at[hot], hv.at[far], kv_send.at[1], kv_recv.at[1], at(0, 0, 1)),
    ]
    gathers, returns = {}, {}
    for step, (dy, dx) in OWNER.items():
        if step == A0:
            continue
        back = next(k for k, at_ in OWNER.items() if at_ == ((NY - dy) % NY, dx))
        first = B0 if step in (B1, B2, B3) else A0
        gathers[step] = remote(
            qt.at[first], qt.at[step], ag_send.at[step], ag_recv.at[step], at((NY - dy) % NY, dx if step == B0 else 0)
        )
        returns[step] = remote(res.at[step], ra.at[back], rs_send.at[step], rs_recv.at[back], at(dy, dx))
    arrivals = {
        step: remote(res.at[step], ra.at[step], rs_send.at[step], rs_recv.at[step], at(0, 1)) for step in returns
    }

    for dz in (1, 3):
        pl.semaphore_signal(far_sem, inc=1, device_id=head_at(0, dz), device_id_type=MESH)
    for step in (B0, A3, A1, A2):
        gathers[step].start()
    local[5].wait()
    local[6].wait()
    for copy in kv_copies:
        copy.start()
    local[8].start()
    local[9].start()

    for copy in local[1:5]:
        copy.wait()
    lane = lax.broadcasted_iota(I32, (2 * seqs, rows), 0)
    pick = seq_at(lax.broadcasted_iota(I32, (2 * seqs, rows), 1) % seqs)
    spread = jnp.where(lane == core * seqs + pick, 1.0, 0.0).astype(BF16)
    used = jnp.dot(used_v[...].astype(F32).astype(BF16), spread, preferred_element_type=F32)
    own_t[pl.ds(0, 8), :] = used
    for step, (dy, dx) in OWNER.items():
        chip = ((y + dy) % NY) * 2 + (xh + dx) % 2
        urow[pl.ds(step, 1), :] = own_t[pl.ds(chip, 1), :]
    lane = lax.broadcasted_iota(I32, (seqs, rows), 0)
    pick = seq_at(lax.broadcasted_iota(I32, (seqs, rows), 1) % seqs)
    spread = jnp.where(lane == pick, 1.0, 0.0).astype(BF16)
    lens = jnp.broadcast_to(len_v[...].astype(F32), (8, seqs)).astype(BF16)
    lrow[...] = jnp.dot(lens, spread, preferred_element_type=F32)
    hot_n = hot_v.shape[1]
    cand = lax.broadcasted_iota(I32, (2 * HOT_CAP, hot_n), 0)
    group = jnp.where(cand < HOT_CAP, me, at(0, 0, 1)["pages"])
    match = hot_v[...] == group * k_hbm.shape[0] + cand % HOT_CAP
    order = lax.broadcasted_iota(I32, (2 * HOT_CAP, hot_n), 1).astype(F32)
    pos[...] = jnp.broadcast_to(
        jnp.min(jnp.where(match, order, 1e9), axis=1, keepdims=True), pos.shape
    )

    qbd[...] = jnp.zeros_like(qbd)

    def set_queries(step):
        qbd[0, pl.ds(0, hd), pl.ds(0, half)] = qt[step, :, pl.ds(0, half)]
        qbd[0, pl.ds(hd, hd), pl.ds(half, half)] = qt[step, :, pl.ds(half, half)]

    def transpose_values(first):
        for j in range(first, first + HOT_CAP):
            for h in range(kvh):
                vt[h, :, pl.ds(j * page, page)] = hv[j, h].T

    transpose_values(0)

    def shared_block(step, slot, previous):
        if step is not None:
            set_queries(step)
            allowed = jnp.where(urow[pl.ds(step, 1), :] > pos[:, pl.ds(0, 1)], 1.0, 0.0)
            sums = jnp.zeros((8, rows), F32)
        parts = [jnp.zeros((hd, half), F32) for _ in range(kvh)]

        def scores(c):
            keys = jnp.concatenate(
                [hk[pl.ds(2 * c, 2), h].reshape(2 * page, hd) for h in range(kvh)], axis=1
            )
            return jnp.dot(keys, qbd[0], preferred_element_type=F32)

        def values(c):
            for h in range(kvh):
                parts[h] = parts[h] + jnp.dot(
                    vt[h, :, pl.ds(2 * c * page, 2 * page)],
                    wt[1 - slot, pl.ds(2 * c * page, 2 * page), pl.ds(h * half, half)],
                    preferred_element_type=F32,
                )

        if step is not None:
            logits = scores(0)
        for c in range(HOT_CAP):
            if previous is not None:
                values(c)
            if step is None:
                continue
            for i in range(2 * page // 16):
                j = (2 * c * page + i * 16) // page
                weight = weights_of(logits[i * 16 : (i + 1) * 16]) * allowed[j : j + 1]
                sums = sums + weight[:8] + weight[8:]
                wt[slot, pl.ds(2 * c * page + i * 16, 16), :] = weight.astype(BF16)
            if c + 1 < HOT_CAP:
                logits = scores(c + 1)
        if step is not None:
            res[step, pl.ds(hd, 16), :] = split_sum(jnp.sum(sums, axis=0, keepdims=True), rows)
        if previous is not None:
            for h in range(kvh):
                res[previous, pl.ds(0, hd), pl.ds(h * half, half)] = parts[h].astype(BF16)

    def page_of(place):
        return jnp.maximum(up_s[0, seq_at(place)] - HOT_CAP, 0)

    def own_scores():
        local[7].wait()
        set_queries(A0)

        def some(g, carry):
            seq_of = lax.broadcasted_iota(I32, (page, rows), 1) % seqs
            tile = own_t[...]
            for i in range(0, 16, 2):
                pages = [page_of(g * 16 + i + j) for j in range(2)]
                keys = jnp.concatenate(
                    [jnp.concatenate([kbuf[u, h] for h in range(kvh)], axis=1) for u in pages], axis=0
                )
                logits = jnp.dot(keys, qbd[0], preferred_element_type=F32)
                for j in range(2):
                    tile = jnp.where(seq_of == g * 16 + i + j, logits[j * page : (j + 1) * page], tile)
            own_t[...] = tile
            return carry

        own_t[...] = jnp.zeros_like(own_t)
        lax.fori_loop(0, seqs // 16, some, 0)

    def own_weights():
        token = lax.broadcasted_iota(I32, (page, rows), 0).astype(F32)
        weight = jnp.where(token < lrow[pl.ds(0, 1), :], weights_of(own_t[...]), 0.0)
        own_t[pl.ds(0, 8), :] = jnp.broadcast_to(jnp.sum(weight, axis=0, keepdims=True), (8, rows))
        own_w[...] = weight.T

    def own_values():
        local[8].wait()

        def some(n, carry):
            row = lax.broadcasted_iota(I32, (8 * heads, page), 0) % 8
            for m in range(4):
                g = n * 4 + m
                weight = jnp.concatenate([own_w[pl.ds(h * seqs + g * 8, 8), :] for h in range(heads)], axis=0)
                left, right = [], []
                for i in range(8):
                    u = page_of(g * 8 + i)
                    left.append(jnp.where(row == i, weight, 0.0).astype(BF16))
                    right.append(jnp.concatenate([vbuf[u, h] for h in range(kvh)], axis=1))
                part = jnp.dot(
                    jnp.concatenate(left, axis=1), jnp.concatenate(right, axis=0), preferred_element_type=F32
                )
                for h in range(heads):
                    own_o[pl.ds(h * seqs + g * 8, 8), :] = part[h * 8 : (h + 1) * 8]
            return carry

        lax.fori_loop(0, seqs // 32, some, 0)

    own_scores()
    own_weights()
    kv_copies[0].wait()
    kv_copies[1].wait()
    transpose_values(HOT_CAP)

    def arrive(step, steps):
        for k in steps:
            @pl.when(step == k)
            def _():
                gathers[k].wait_recv()
                if k == B0:
                    for n in (B3, B1, B2):
                        gathers[n].start()

    def send_back(step, steps):
        for k in steps:
            @pl.when(step == k)
            def _():
                returns[k].start()

    def two_steps(n, carry):
        step = 2 * n + 1
        arrive(step, (1, 3, 5))
        shared_block(step, 1, step - 1)
        send_back(step - 1, (0, 2, 4))
        arrive(step + 1, (2, 4, 6))
        shared_block(step + 1, 0, step)
        send_back(step, (1, 3, 5))
        return carry

    gathers[0].wait_recv()
    shared_block(0, 0, None)
    lax.fori_loop(0, 3, two_steps, 0)
    shared_block(7, 1, 6)
    returns[6].start()
    shared_block(None, 0, 7)
    own_values()

    def summed(pieces):
        return sum(piece[...].astype(F32) for piece in pieces)

    own_num = [own_o[pl.ds(h * half, half), pl.ds(h * hd, hd)].T for h in range(kvh)]
    for copy in arrivals.values():
        copy.wait_recv()
    whole = summed([res.at[A0], *(ra.at[k] for k in arrivals)])
    total = jnp.sum(whole[hd:], axis=0, keepdims=True) + own_t[pl.ds(0, 1), :]
    for h in range(kvh):
        lanes = slice(h * half, (h + 1) * half)
        attended = ((whole[:hd, lanes] + own_num[h]) / total[:, lanes]).T.astype(BF16)
        for g in range(half // seqs):
            head = h * (half // seqs) + g
            att[:, pl.ds(head * hd, hd)] = attended[g * seqs : (g + 1) * seqs]

    local[9].wait()
    block = seqs // NZ
    width = w_v.shape[1] // CHUNKS
    relayed, plain, joined, across = {}, {}, {}, {}
    order = [k // 2 + (k % 2) * (CHUNKS // 2) for k in range(CHUNKS)]
    pl.semaphore_wait(far_sem, 2)
    for k in order:
        via, other = (1, 3) if k < CHUNKS // 2 else (3, 1)
        cols = pl.ds(k * width, width)
        piece = jnp.dot(att[...], w_v[:, cols], preferred_element_type=F32).astype(BF16)
        for i in range(NZ):
            for j in range(2):
                pz[i, j, :, cols] = piece[i * block + j * 8 : i * block + j * 8 + 8]

        def to_sum(src, dx, dz, n):
            slot = 4 if dz == 0 else 2 * dx + dz // 2
            return remote(
                src, zr.at[slot, :, cols], z_send.at[n * CHUNKS + k], z_recv.at[n * CHUNKS + k], head_at(dx, dz)
            )

        relayed[k] = remote(pz.at[(z + 2) % NZ, :, :, cols], zt.at[:, :, cols], z_send.at[k], z_recv.at[k], head_at(0, via))
        plain[k] = [to_sum(pz.at[(z + other) % NZ, (xl + dx) % 2, :, cols], dx, other, 1 + dx) for dx in range(2)]
        joined[k] = [to_sum(zj.at[(xl + dx) % 2, :, cols], dx, via, 3 + dx) for dx in range(2)]
        across[k] = [to_sum(pz.at[z, 1 - xl, :, cols], 1, 0, 5)]
        for copy in (relayed[k], *plain[k], *across[k]):
            copy.start()
    for k in order:
        via = 1 if k < CHUNKS // 2 else 3
        cols = pl.ds(k * width, width)
        relayed[k].wait_recv()
        for j in range(2):
            zj[j, :, cols] = (pz[(z + via) % NZ, j, :, cols].astype(F32) + zt[j, :, cols].astype(F32)).astype(BF16)
        for copy in joined[k]:
            copy.start()
    square = jnp.zeros((block // 2, 1), F32)
    for k in order:
        cols = pl.ds(k * width, width)
        for copy in (*plain[k], *across[k]):
            copy.wait_recv()
        for copy in joined[k]:
            copy.wait_recv()
        projected = pz[z, xl, :, cols].astype(F32)
        for i in range(5):
            projected = projected + zr[i, :, cols].astype(F32)
        near_sum[:, cols] = projected
        square = square + jnp.sum(projected * projected, axis=1, keepdims=True)
    out_ref[...] = near_sum[...] / jnp.sqrt(square / w_v.shape[1] + epsilon)

    sent = [*gathers.values(), *returns.values(), *relayed.values()]
    for copy in sum([*plain.values(), *joined.values(), *across.values()], sent):
        copy.wait_send()


def layer(queries, keys, values, hot_pages, hot_used, user_pages, lengths, o_weight):
    seqs, heads, hd = queries.shape
    pages, kvh, page, _ = keys.shape
    rows = seqs * heads
    width = o_weight.shape[1]
    vmem = pltpu.VMEM
    return pl.pallas_call(
        layer_kernel,
        out_shape=jax.ShapeDtypeStruct((seqs // 8, width), F32),
        in_specs=[pl.BlockSpec(memory_space=pl.ANY)] * 8,
        out_specs=pl.BlockSpec(memory_space=pltpu.VMEM),
        scratch_shapes=[
            vmem((rows, hd), BF16),
            vmem((1, hot_pages.shape[0]), I32),
            vmem((hot_used.shape[0] // 128, 128), I32),
            vmem((1, seqs), I32),
            pltpu.SMEM((1, seqs), I32),
            vmem((pages - HOT_CAP, kvh, page, hd), BF16),
            vmem((pages - HOT_CAP, kvh, page, hd), BF16),
            vmem((2 * HOT_CAP, kvh, page, hd), BF16),
            vmem((2 * HOT_CAP, kvh, page, hd), BF16),
            vmem((kvh, hd, 2 * HOT_CAP * page), BF16),
            vmem((8, hd, rows), BF16),
            vmem((1, kvh * hd, rows), BF16),
            vmem((8, rows), F32),
            vmem((8, rows), F32),
            vmem((2 * HOT_CAP, 128), F32),
            vmem((2, 2 * HOT_CAP * page, rows), BF16),
            vmem((8, hd + 16, rows), BF16),
            vmem((7, hd + 16, rows), BF16),
            vmem((page, rows), F32),
            vmem((rows, page), F32),
            vmem((rows, kvh * hd), F32),
            vmem(o_weight.shape, BF16),
            vmem((seqs, heads * hd), BF16),
            vmem((NZ, 2, 8, width), BF16),
            vmem((2, 8, width), BF16),
            vmem((2, 8, width), BF16),
            vmem((5, 8, width), BF16),
            vmem((seqs // 8, width), F32),
            pltpu.SemaphoreType.DMA((10,)),
            pltpu.SemaphoreType.DMA((6 * CHUNKS,)),
            pltpu.SemaphoreType.DMA((6 * CHUNKS,)),
            pltpu.SemaphoreType.DMA((2,)),
            pltpu.SemaphoreType.DMA((2,)),
            pltpu.SemaphoreType.DMA((7,)),
            pltpu.SemaphoreType.DMA((7,)),
            pltpu.SemaphoreType.DMA((7,)),
            pltpu.SemaphoreType.DMA((7,)),
            pltpu.SemaphoreType.REGULAR,
        ],
        compiler_params=pltpu.CompilerParams(
            collective_id=0, has_side_effects=True, vmem_limit_bytes=64_500_000
        ),
        name="layer",
    )(
        queries.reshape(rows, hd),
        keys,
        values,
        hot_pages.reshape(1, -1),
        hot_used.reshape(-1, 128),
        user_pages.reshape(1, -1),
        lengths.reshape(1, -1),
        o_weight,
    )


def per_device(
    queries, keys, values, hot_pages, hot_used, user_pages, lengths, o_weight, residual, norm_gain
):
    normed = layer(queries, keys, values, hot_pages, hot_used, user_pages, lengths, o_weight)
    return (residual.astype(F32) + normed * norm_gain[None, :]).astype(BF16)


def solution(mesh):
    in_specs = (
        P("pages", "heads", None),
        P("pages", "heads", None, None),
        P("pages", "heads", None, None),
        P(),
        P(),
        P("pages", None),
        P("pages"),
        P("heads", None),
        P(("pages", "heads"), None),
        P(),
    )
    out_specs = P(("pages", "heads"), None)
    return jax.shard_map(
        per_device, mesh=mesh, in_specs=in_specs, out_specs=out_specs, check_vma=False
    )
```

```python
import functools
import math

import jax
import jax.numpy as jnp
from jax import lax
from jax.experimental import pallas as pl
from jax.experimental.pallas import tpu as pltpu
from jax.sharding import PartitionSpec as P

HOT_CAP = 8
soft_cap = 50.0
score_scale = 1.0 / 12.0
epsilon = 1e-06
NY = 4
NZ = 4
CHUNKS = 6
F32, BF16, I32 = jnp.float32, jnp.bfloat16, jnp.int32
MESH = pl.DeviceIdType.MESH

A3, B0, A1, B3, A2, B1, B2, A0 = range(8)
OWNER = {A3: (3, 0), A1: (1, 0), A2: (2, 0), B0: (0, 1), B3: (3, 1), B1: (1, 1), B2: (2, 1), A0: (0, 0)}


def weights_of(logits):
    return jnp.exp2(jnp.tanh(logits * (score_scale / soft_cap)) * (soft_cap * math.log2(math.e)))


def split_sum(totals, rows):
    high = totals.astype(BF16).astype(F32)
    row = lax.broadcasted_iota(I32, (16, rows), 0)
    return jnp.where(row == 0, high, jnp.where(row == 1, totals - high, 0.0)).astype(BF16)


def layer_kernel(
    q_hbm, k_hbm, v_hbm, hot_hbm, used_hbm, up_hbm, len_hbm, w_hbm, out_ref,
    q_v, hot_v, used_v, len_v, up_s, kbuf, vbuf, hk, hv, vt, qt, qbd, urow, lrow, pos,
    wt, res, ra, own_t, own_w, own_o,
    w_v, att, pz, zt, zj, zr, near_sum,
    in_sem, z_send, z_recv, kv_send, kv_recv, ag_send, ag_recv, rs_send, rs_recv, far_sem, diag_sem,
):
    seqs = len_v.shape[1]
    kvh, page, hd = hk.shape[1:]
    rows = q_v.shape[0]
    half = rows // kvh
    me = lax.axis_index("pages")
    y, xh, core = me // 4, (me // 2) % 2, me % 2

    member = lax.axis_index("heads")
    xl, z = member // NZ, member % NZ

    def head_at(dx, dz):
        return {"heads": ((xl + dx) % 2) * NZ + (z + dz) % NZ}

    def seq_at(place):
        return ((place // 8) % 2) * (seqs // 2) + (place // 16) * 8 + place % 8

    def at(dy, dx=0, dc=0):
        return {"pages": ((y + dy) % NY) * 4 + ((xh + dx) % 2) * 2 + (core + dc) % 2}

    def remote(src, dst, send, recv, target):
        return pltpu.make_async_remote_copy(
            src_ref=src, dst_ref=dst, send_sem=send, recv_sem=recv, device_id=target, device_id_type=MESH
        )

    own = pl.ds(HOT_CAP, k_hbm.shape[0] - HOT_CAP)
    hot = pl.ds(0, HOT_CAP)
    local = [
        pltpu.make_async_copy(q_hbm, q_v, in_sem.at[0]),
        pltpu.make_async_copy(hot_hbm, hot_v, in_sem.at[1]),
        pltpu.make_async_copy(used_hbm, used_v, in_sem.at[2]),
        pltpu.make_async_copy(len_hbm, len_v, in_sem.at[3]),
        pltpu.make_async_copy(up_hbm, up_s, in_sem.at[4]),
        pltpu.make_async_copy(k_hbm.at[hot], hk.at[hot], in_sem.at[5]),
        pltpu.make_async_copy(v_hbm.at[hot], hv.at[hot], in_sem.at[6]),
        pltpu.make_async_copy(k_hbm.at[own], kbuf, in_sem.at[7]),
        pltpu.make_async_copy(v_hbm.at[own], vbuf, in_sem.at[8]),
        pltpu.make_async_copy(w_hbm, w_v, in_sem.at[9]),
    ]
    for copy in local[:8]:
        copy.start()

    barrier = pltpu.get_barrier_semaphore()
    peers = [at(1), at(2), at(3), at(0, 1), at(0, 0, 1)]
    peers += [head_at(0, 1), head_at(0, 2), head_at(0, 3), head_at(1, 0)]
    for peer in peers:
        pl.semaphore_signal(barrier, inc=1, device_id=peer, device_id_type=MESH)

    local[0].wait()
    r = lax.broadcasted_iota(I32, (rows, rows), 0)
    col = lax.broadcasted_iota(I32, (rows, rows), 1)
    heads = rows // seqs
    perm = jnp.where(col == seq_at(r % seqs) * heads + r // seqs, 1.0, 0.0).astype(BF16)
    q_rows = jnp.dot(perm, q_v[...], preferred_element_type=F32)
    qt[A0] = q_rows.T.astype(BF16)

    pl.semaphore_wait(barrier, len(peers))

    far = pl.ds(HOT_CAP, HOT_CAP)
    kv_copies = [
        remote(hk.at[hot], hk.at[far], kv_send.at[0], kv_recv.at[0], at(0, 0, 1)),
        remote(hv.at[hot], hv.at[far], kv_send.at[1], kv_recv.at[1], at(0, 0, 1)),
    ]
    gathers, returns = {}, {}
    for step, (dy, dx) in OWNER.items():
        if step == A0:
            continue
        back = next(k for k, at_ in OWNER.items() if at_ == ((NY - dy) % NY, dx))
        gathers[step] = remote(qt.at[A0], qt.at[step], ag_send.at[step], ag_recv.at[step], at((NY - dy) % NY, dx))
        returns[step] = remote(res.at[step], ra.at[back], rs_send.at[step], rs_recv.at[back], at(dy, dx))
    arrivals = {
        step: remote(res.at[step], ra.at[step], rs_send.at[step], rs_recv.at[step], at(0, 1)) for step in returns
    }

    pl.semaphore_signal(far_sem, inc=1, device_id=at(0, 1), device_id_type=MESH)
    for dz in (1, 3):
        pl.semaphore_signal(diag_sem, inc=1, device_id=head_at(0, dz), device_id_type=MESH)
    for step in (B0, A3, A1, A2):
        gathers[step].start()
    local[5].wait()
    local[6].wait()
    for copy in kv_copies:
        copy.start()
    local[8].start()
    local[9].start()

    for copy in local[1:5]:
        copy.wait()
    lane = lax.broadcasted_iota(I32, (2 * seqs, rows), 0)
    pick = seq_at(lax.broadcasted_iota(I32, (2 * seqs, rows), 1) % seqs)
    spread = jnp.where(lane == core * seqs + pick, 1.0, 0.0).astype(BF16)
    used = jnp.dot(used_v[...].astype(F32).astype(BF16), spread, preferred_element_type=F32)
    own_t[pl.ds(0, 8), :] = used
    for step, (dy, dx) in OWNER.items():
        chip = ((y + dy) % NY) * 2 + (xh + dx) % 2
        urow[pl.ds(step, 1), :] = own_t[pl.ds(chip, 1), :]
    lane = lax.broadcasted_iota(I32, (seqs, rows), 0)
    pick = seq_at(lax.broadcasted_iota(I32, (seqs, rows), 1) % seqs)
    spread = jnp.where(lane == pick, 1.0, 0.0).astype(BF16)
    lens = jnp.broadcast_to(len_v[...].astype(F32), (8, seqs)).astype(BF16)
    lrow[...] = jnp.dot(lens, spread, preferred_element_type=F32)
    hot_n = hot_v.shape[1]
    cand = lax.broadcasted_iota(I32, (2 * HOT_CAP, hot_n), 0)
    group = jnp.where(cand < HOT_CAP, me, at(0, 0, 1)["pages"])
    match = hot_v[...] == group * k_hbm.shape[0] + cand % HOT_CAP
    order = lax.broadcasted_iota(I32, (2 * HOT_CAP, hot_n), 1).astype(F32)
    pos[...] = jnp.broadcast_to(
        jnp.min(jnp.where(match, order, 1e9), axis=1, keepdims=True), pos.shape
    )

    qbd[...] = jnp.zeros_like(qbd)

    def set_queries(step):
        qbd[0, pl.ds(0, hd), pl.ds(0, half)] = qt[step, :, pl.ds(0, half)]
        qbd[0, pl.ds(hd, hd), pl.ds(half, half)] = qt[step, :, pl.ds(half, half)]

    def transpose_values(first):
        for j in range(first, first + HOT_CAP):
            for h in range(kvh):
                vt[h, :, pl.ds(j * page, page)] = hv[j, h].T

    transpose_values(0)

    def shared_block(step, slot, previous):
        if step is not None:
            set_queries(step)
            allowed = jnp.where(urow[pl.ds(step, 1), :] > pos[:, pl.ds(0, 1)], 1.0, 0.0)
            sums = jnp.zeros((8, rows), F32)
        parts = [jnp.zeros((hd, half), F32) for _ in range(kvh)]

        def scores(c):
            keys = jnp.concatenate(
                [hk[pl.ds(2 * c, 2), h].reshape(2 * page, hd) for h in range(kvh)], axis=1
            )
            return jnp.dot(keys, qbd[0], preferred_element_type=F32)

        def values(c):
            for h in range(kvh):
                parts[h] = parts[h] + jnp.dot(
                    vt[h, :, pl.ds(2 * c * page, 2 * page)],
                    wt[1 - slot, pl.ds(2 * c * page, 2 * page), pl.ds(h * half, half)],
                    preferred_element_type=F32,
                )

        if step is not None:
            logits = scores(0)
        for c in range(HOT_CAP):
            if previous is not None:
                values(c)
            if step is None:
                continue
            for i in range(2 * page // 16):
                j = (2 * c * page + i * 16) // page
                weight = weights_of(logits[i * 16 : (i + 1) * 16]) * allowed[j : j + 1]
                sums = sums + weight[:8] + weight[8:]
                wt[slot, pl.ds(2 * c * page + i * 16, 16), :] = weight.astype(BF16)
            if c + 1 < HOT_CAP:
                logits = scores(c + 1)
        if step is not None:
            res[step, pl.ds(hd, 16), :] = split_sum(jnp.sum(sums, axis=0, keepdims=True), rows)
        if previous is not None:
            for h in range(kvh):
                res[previous, pl.ds(0, hd), pl.ds(h * half, half)] = parts[h].astype(BF16)

    def page_of(place):
        return jnp.maximum(up_s[0, seq_at(place)] - HOT_CAP, 0)

    def own_scores(first, last):
        def some(g, carry):
            seq_of = lax.broadcasted_iota(I32, (page, rows), 1) % seqs
            tile = own_t[...]
            for i in range(0, 16, 2):
                pages = [page_of(g * 16 + i + j) for j in range(2)]
                keys = jnp.concatenate(
                    [jnp.concatenate([kbuf[u, h] for h in range(kvh)], axis=1) for u in pages], axis=0
                )
                logits = jnp.dot(keys, qbd[0], preferred_element_type=F32)
                for j in range(2):
                    tile = jnp.where(seq_of == g * 16 + i + j, logits[j * page : (j + 1) * page], tile)
            own_t[...] = tile
            return carry

        lax.fori_loop(first, last, some, 0)

    def own_weights():
        token = lax.broadcasted_iota(I32, (page, rows), 0).astype(F32)
        weight = jnp.where(token < lrow[pl.ds(0, 1), :], weights_of(own_t[...]), 0.0)
        own_t[pl.ds(0, 8), :] = jnp.broadcast_to(jnp.sum(weight, axis=0, keepdims=True), (8, rows))
        own_w[...] = weight.T

    def own_values():
        local[8].wait()

        def some(n, carry):
            row = lax.broadcasted_iota(I32, (8 * heads, page), 0) % 8
            for m in range(4):
                g = n * 4 + m
                weight = jnp.concatenate([own_w[pl.ds(h * seqs + g * 8, 8), :] for h in range(heads)], axis=0)
                left, right = [], []
                for i in range(8):
                    u = page_of(g * 8 + i)
                    left.append(jnp.where(row == i, weight, 0.0).astype(BF16))
                    right.append(jnp.concatenate([vbuf[u, h] for h in range(kvh)], axis=1))
                part = jnp.dot(
                    jnp.concatenate(left, axis=1), jnp.concatenate(right, axis=0), preferred_element_type=F32
                )
                for h in range(heads):
                    own_o[pl.ds(h * seqs + g * 8, 8), :] = part[h * 8 : (h + 1) * 8]
            return carry

        lax.fori_loop(0, seqs // 32, some, 0)

    set_queries(A0)
    own_t[...] = jnp.zeros_like(own_t)
    local[7].wait()
    own_scores(0, seqs // 32)
    pl.semaphore_wait(far_sem, 1)
    for step in (B3, B1, B2):
        gathers[step].start()
    kv_copies[0].wait()
    kv_copies[1].wait()
    transpose_values(HOT_CAP)

    def arrive(step, steps):
        for k in steps:
            @pl.when(step == k)
            def _():
                gathers[k].wait_recv()

    def send_back(step, steps):
        for k in steps:
            @pl.when(step == k)
            def _():
                returns[k].start()

    def two_steps(n, carry):
        step = 2 * n + 1
        arrive(step, (1, 3, 5))
        shared_block(step, 1, step - 1)
        send_back(step - 1, (0, 2, 4))
        arrive(step + 1, (2, 4, 6))
        shared_block(step + 1, 0, step)
        send_back(step, (1, 3, 5))
        return carry

    gathers[0].wait_recv()
    shared_block(0, 0, None)
    lax.fori_loop(0, 3, two_steps, 0)
    shared_block(7, 1, 6)
    returns[6].start()
    shared_block(None, 0, 7)
    own_scores(seqs // 32, seqs // 16)
    own_weights()
    own_values()

    def summed(pieces):
        return sum(piece[...].astype(F32) for piece in pieces)

    own_num = [own_o[pl.ds(h * half, half), pl.ds(h * hd, hd)].T for h in range(kvh)]
    for copy in arrivals.values():
        copy.wait_recv()
    whole = summed([res.at[A0], *(ra.at[k] for k in arrivals)])
    total = jnp.sum(whole[hd:], axis=0, keepdims=True) + own_t[pl.ds(0, 1), :]
    for h in range(kvh):
        lanes = slice(h * half, (h + 1) * half)
        attended = ((whole[:hd, lanes] + own_num[h]) / total[:, lanes]).T.astype(BF16)
        for g in range(half // seqs):
            head = h * (half // seqs) + g
            att[:, pl.ds(head * hd, hd)] = attended[g * seqs : (g + 1) * seqs]

    local[9].wait()
    block = seqs // NZ
    width = w_v.shape[1] // CHUNKS
    relayed, plain, joined, across = {}, {}, {}, {}
    order = [k // 2 + (k % 2) * (CHUNKS // 2) for k in range(CHUNKS)]
    pl.semaphore_wait(diag_sem, 2)
    for k in order:
        via, other = (1, 3) if k < CHUNKS // 2 else (3, 1)
        cols = pl.ds(k * width, width)
        piece = jnp.dot(att[...], w_v[:, cols], preferred_element_type=F32).astype(BF16)
        for i in range(NZ):
            for j in range(2):
                pz[i, j, :, cols] = piece[i * block + j * 8 : i * block + j * 8 + 8]

        def to_sum(src, dx, dz, n):
            slot = 4 if dz == 0 else 2 * dx + dz // 2
            return remote(
                src, zr.at[slot, :, cols], z_send.at[n * CHUNKS + k], z_recv.at[n * CHUNKS + k], head_at(dx, dz)
            )

        relayed[k] = remote(pz.at[(z + 2) % NZ, :, :, cols], zt.at[:, :, cols], z_send.at[k], z_recv.at[k], head_at(0, via))
        plain[k] = [to_sum(pz.at[(z + other) % NZ, (xl + dx) % 2, :, cols], dx, other, 1 + dx) for dx in range(2)]
        joined[k] = [to_sum(zj.at[(xl + dx) % 2, :, cols], dx, via, 3 + dx) for dx in range(2)]
        across[k] = [to_sum(pz.at[z, 1 - xl, :, cols], 1, 0, 5)]
        relayed[k].start()
    for k in order:
        for copy in (*plain[k], *across[k]):
            copy.start()
    for k in order:
        via = 1 if k < CHUNKS // 2 else 3
        cols = pl.ds(k * width, width)
        relayed[k].wait_recv()
        for j in range(2):
            zj[j, :, cols] = (pz[(z + via) % NZ, j, :, cols].astype(F32) + zt[j, :, cols].astype(F32)).astype(BF16)
        for copy in joined[k]:
            copy.start()
    square = jnp.zeros((block // 2, 1), F32)
    for k in order:
        cols = pl.ds(k * width, width)
        for copy in (*plain[k], *across[k]):
            copy.wait_recv()
        for copy in joined[k]:
            copy.wait_recv()
        projected = pz[z, xl, :, cols].astype(F32)
        for i in range(5):
            projected = projected + zr[i, :, cols].astype(F32)
        near_sum[:, cols] = projected
        square = square + jnp.sum(projected * projected, axis=1, keepdims=True)
    out_ref[...] = near_sum[...] / jnp.sqrt(square / w_v.shape[1] + epsilon)

    sent = [*gathers.values(), *returns.values(), *relayed.values()]
    for copy in sum([*plain.values(), *joined.values(), *across.values()], sent):
        copy.wait_send()


def layer(queries, keys, values, hot_pages, hot_used, user_pages, lengths, o_weight):
    seqs, heads, hd = queries.shape
    pages, kvh, page, _ = keys.shape
    rows = seqs * heads
    width = o_weight.shape[1]
    vmem = pltpu.VMEM
    return pl.pallas_call(
        layer_kernel,
        out_shape=pltpu.VMEM((seqs // 8, width), F32),
        in_specs=[pl.BlockSpec(memory_space=pl.ANY)] * 8,
        out_specs=pl.BlockSpec(memory_space=pltpu.VMEM),
        scratch_shapes=[
            vmem((rows, hd), BF16),
            vmem((1, hot_pages.shape[0]), I32),
            vmem((hot_used.shape[0] // 128, 128), I32),
            vmem((1, seqs), I32),
            pltpu.SMEM((1, seqs), I32),
            vmem((pages - HOT_CAP, kvh, page, hd), BF16),
            vmem((pages - HOT_CAP, kvh, page, hd), BF16),
            vmem((2 * HOT_CAP, kvh, page, hd), BF16),
            vmem((2 * HOT_CAP, kvh, page, hd), BF16),
            vmem((kvh, hd, 2 * HOT_CAP * page), BF16),
            vmem((8, hd, rows), BF16),
            vmem((1, kvh * hd, rows), BF16),
            vmem((8, rows), F32),
            vmem((8, rows), F32),
            vmem((2 * HOT_CAP, 128), F32),
            vmem((2, 2 * HOT_CAP * page, rows), BF16),
            vmem((8, hd + 16, rows), BF16),
            vmem((7, hd + 16, rows), BF16),
            vmem((page, rows), F32),
            vmem((rows, page), F32),
            vmem((rows, kvh * hd), F32),
            vmem(o_weight.shape, BF16),
            vmem((seqs, heads * hd), BF16),
            vmem((NZ, 2, 8, width), BF16),
            vmem((2, 8, width), BF16),
            vmem((2, 8, width), BF16),
            vmem((5, 8, width), BF16),
            vmem((seqs // 8, width), F32),
            pltpu.SemaphoreType.DMA((10,)),
            pltpu.SemaphoreType.DMA((6 * CHUNKS,)),
            pltpu.SemaphoreType.DMA((6 * CHUNKS,)),
            pltpu.SemaphoreType.DMA((2,)),
            pltpu.SemaphoreType.DMA((2,)),
            pltpu.SemaphoreType.DMA((7,)),
            pltpu.SemaphoreType.DMA((7,)),
            pltpu.SemaphoreType.DMA((7,)),
            pltpu.SemaphoreType.DMA((7,)),
            pltpu.SemaphoreType.REGULAR,
            pltpu.SemaphoreType.REGULAR,
        ],
        compiler_params=pltpu.CompilerParams(
            collective_id=0, has_side_effects=True, vmem_limit_bytes=64_500_000
        ),
        name="layer",
    )(
        queries.reshape(rows, hd),
        keys,
        values,
        hot_pages.reshape(1, -1),
        hot_used.reshape(-1, 128),
        user_pages.reshape(1, -1),
        lengths.reshape(1, -1),
        o_weight,
    )


def per_device(
    queries, keys, values, hot_pages, hot_used, user_pages, lengths, o_weight, residual, norm_gain
):
    normed = layer(queries, keys, values, hot_pages, hot_used, user_pages, lengths, o_weight)
    return (residual.astype(F32) + normed * norm_gain[None, :]).astype(BF16)


def solution(mesh):
    in_specs = (
        P("pages", "heads", None),
        P("pages", "heads", None, None),
        P("pages", "heads", None, None),
        P(),
        P(),
        P("pages", None),
        P("pages"),
        P("heads", None),
        P(("pages", "heads"), None),
        P(),
    )
    out_specs = P(("pages", "heads"), None)
    return jax.shard_map(
        per_device, mesh=mesh, in_specs=in_specs, out_specs=out_specs, check_vma=False
    )
```

```python
import functools
import math

import jax
import jax.numpy as jnp
from jax import lax
from jax.experimental import pallas as pl
from jax.experimental.pallas import tpu as pltpu
from jax.sharding import PartitionSpec as P

HOT_CAP = 8
soft_cap = 50.0
score_scale = 1.0 / 12.0
epsilon = 1e-06
NY = 4
NZ = 4
CHUNKS = 6
F32, BF16, I32 = jnp.float32, jnp.bfloat16, jnp.int32
MESH = pl.DeviceIdType.MESH

A3, B0, A1, B3, A2, B1, B2, A0 = range(8)
OWNER = {A3: (3, 0), A1: (1, 0), A2: (2, 0), B0: (0, 1), B3: (3, 1), B1: (1, 1), B2: (2, 1), A0: (0, 0)}


def weights_of(logits):
    return jnp.exp2(jnp.tanh(logits * (score_scale / soft_cap)) * (soft_cap * math.log2(math.e)))


def split_sum(totals, rows):
    high = totals.astype(BF16).astype(F32)
    row = lax.broadcasted_iota(I32, (16, rows), 0)
    return jnp.where(row == 0, high, jnp.where(row == 1, totals - high, 0.0)).astype(BF16)


def layer_kernel(
    q_hbm, k_hbm, v_hbm, hot_hbm, used_hbm, up_hbm, len_hbm, w_hbm, out_ref,
    q_v, hot_v, used_v, len_v, up_s, kbuf, vbuf, hk, hv, vt, qt, qbd, urow, lrow, pos,
    wt, res, ra, own_t, own_w, own_o,
    w_v, att, pz, zt, zj, zr, near_sum,
    in_sem, z_send, z_recv, kv_send, kv_recv, ag_send, ag_recv, rs_send, rs_recv, far_sem, diag_sem,
):
    seqs = len_v.shape[1]
    kvh, page, hd = hk.shape[1:]
    rows = q_v.shape[0]
    half = rows // kvh
    me = lax.axis_index("pages")
    y, xh, core = me // 4, (me // 2) % 2, me % 2

    member = lax.axis_index("heads")
    xl, z = member // NZ, member % NZ

    def head_at(dx, dz):
        return {"heads": ((xl + dx) % 2) * NZ + (z + dz) % NZ}

    def seq_at(place):
        return ((place // 8) % 2) * (seqs // 2) + (place // 16) * 8 + place % 8

    def at(dy, dx=0, dc=0):
        return {"pages": ((y + dy) % NY) * 4 + ((xh + dx) % 2) * 2 + (core + dc) % 2}

    def remote(src, dst, send, recv, target):
        return pltpu.make_async_remote_copy(
            src_ref=src, dst_ref=dst, send_sem=send, recv_sem=recv, device_id=target, device_id_type=MESH
        )

    own = pl.ds(HOT_CAP, k_hbm.shape[0] - HOT_CAP)
    hot = pl.ds(0, HOT_CAP)
    def settle(like, semaphore):
        pltpu.make_async_copy(like, like, semaphore).wait()

    local = [
        pltpu.make_async_copy(q_hbm, q_v, in_sem.at[0]),
        pltpu.make_async_copy(hot_hbm, hot_v, in_sem.at[1]),
        pltpu.make_async_copy(used_hbm, used_v, in_sem.at[2]),
        pltpu.make_async_copy(len_hbm, len_v, in_sem.at[3]),
        pltpu.make_async_copy(up_hbm, up_s, in_sem.at[4]),
        pltpu.make_async_copy(k_hbm.at[hot], hk.at[hot], in_sem.at[5]),
        pltpu.make_async_copy(v_hbm.at[hot], hv.at[hot], in_sem.at[6]),
        pltpu.make_async_copy(k_hbm.at[own], kbuf, in_sem.at[7]),
        pltpu.make_async_copy(v_hbm.at[own], vbuf, in_sem.at[8]),
        pltpu.make_async_copy(w_hbm, w_v, in_sem.at[9]),
    ]
    for copy in local[:8]:
        copy.start()

    barrier = pltpu.get_barrier_semaphore()
    peers = [at(1), at(2), at(3), at(0, 1), at(0, 0, 1)]
    peers += [head_at(0, 1), head_at(0, 2), head_at(0, 3), head_at(1, 0)]
    for peer in peers:
        pl.semaphore_signal(barrier, inc=1, device_id=peer, device_id_type=MESH)

    local[0].wait()
    r = lax.broadcasted_iota(I32, (rows, rows), 0)
    col = lax.broadcasted_iota(I32, (rows, rows), 1)
    heads = rows // seqs
    perm = jnp.where(col == seq_at(r % seqs) * heads + r // seqs, 1.0, 0.0).astype(BF16)
    q_rows = jnp.dot(perm, q_v[...], preferred_element_type=F32)
    qt[A0] = q_rows.T.astype(BF16)

    pl.semaphore_wait(barrier, len(peers))

    far = pl.ds(HOT_CAP, HOT_CAP)
    kv_copies = [
        remote(hk.at[hot], hk.at[far], kv_send, kv_recv.at[0], at(0, 0, 1)),
        remote(hv.at[hot], hv.at[far], kv_send, kv_recv.at[1], at(0, 0, 1)),
    ]
    gathers, returns = {}, {}
    for step, (dy, dx) in OWNER.items():
        if step == A0:
            continue
        back = next(k for k, at_ in OWNER.items() if at_ == ((NY - dy) % NY, dx))
        gathers[step] = remote(qt.at[A0], qt.at[step], ag_send, ag_recv.at[step], at((NY - dy) % NY, dx))
        returns[step] = remote(res.at[step], ra.at[back], rs_send, rs_recv.at[back], at(dy, dx))
    arrivals = {
        step: remote(res.at[step], ra.at[step], rs_send, rs_recv.at[step], at(0, 1)) for step in returns
    }

    pl.semaphore_signal(far_sem, inc=1, device_id=at(0, 1), device_id_type=MESH)
    for dz in (1, 3):
        pl.semaphore_signal(diag_sem, inc=1, device_id=head_at(0, dz), device_id_type=MESH)
    for step in (B0, A3, A1, A2):
        gathers[step].start()
    local[5].wait()
    local[6].wait()
    for copy in kv_copies:
        copy.start()
    local[8].start()
    local[9].start()

    for copy in local[1:5]:
        copy.wait()
    lane = lax.broadcasted_iota(I32, (2 * seqs, rows), 0)
    pick = seq_at(lax.broadcasted_iota(I32, (2 * seqs, rows), 1) % seqs)
    spread = jnp.where(lane == core * seqs + pick, 1.0, 0.0).astype(BF16)
    used = jnp.dot(used_v[...].astype(F32).astype(BF16), spread, preferred_element_type=F32)
    own_t[pl.ds(0, 8), :] = used
    for step, (dy, dx) in OWNER.items():
        chip = ((y + dy) % NY) * 2 + (xh + dx) % 2
        urow[pl.ds(step, 1), :] = own_t[pl.ds(chip, 1), :]
    lane = lax.broadcasted_iota(I32, (seqs, rows), 0)
    pick = seq_at(lax.broadcasted_iota(I32, (seqs, rows), 1) % seqs)
    spread = jnp.where(lane == pick, 1.0, 0.0).astype(BF16)
    lens = jnp.broadcast_to(len_v[...].astype(F32), (8, seqs)).astype(BF16)
    lrow[...] = jnp.dot(lens, spread, preferred_element_type=F32)
    hot_n = hot_v.shape[1]
    cand = lax.broadcasted_iota(I32, (2 * HOT_CAP, hot_n), 0)
    group = jnp.where(cand < HOT_CAP, me, at(0, 0, 1)["pages"])
    match = hot_v[...] == group * k_hbm.shape[0] + cand % HOT_CAP
    order = lax.broadcasted_iota(I32, (2 * HOT_CAP, hot_n), 1).astype(F32)
    pos[...] = jnp.broadcast_to(
        jnp.min(jnp.where(match, order, 1e9), axis=1, keepdims=True), pos.shape
    )

    qbd[...] = jnp.zeros_like(qbd)

    def set_queries(step):
        qbd[0, pl.ds(0, hd), pl.ds(0, half)] = qt[step, :, pl.ds(0, half)]
        qbd[0, pl.ds(hd, hd), pl.ds(half, half)] = qt[step, :, pl.ds(half, half)]

    def transpose_values(first):
        for j in range(first, first + HOT_CAP):
            for h in range(kvh):
                vt[h, :, pl.ds(j * page, page)] = hv[j, h].T

    transpose_values(0)

    def shared_block(step, slot, previous):
        if step is not None:
            set_queries(step)
            allowed = jnp.where(urow[pl.ds(step, 1), :] > pos[:, pl.ds(0, 1)], 1.0, 0.0)
            sums = jnp.zeros((8, rows), F32)
        parts = [jnp.zeros((hd, half), F32) for _ in range(kvh)]

        def scores(c):
            keys = jnp.concatenate(
                [hk[pl.ds(2 * c, 2), h].reshape(2 * page, hd) for h in range(kvh)], axis=1
            )
            return jnp.dot(keys, qbd[0], preferred_element_type=F32)

        def values(c):
            for h in range(kvh):
                parts[h] = parts[h] + jnp.dot(
                    vt[h, :, pl.ds(2 * c * page, 2 * page)],
                    wt[1 - slot, pl.ds(2 * c * page, 2 * page), pl.ds(h * half, half)],
                    preferred_element_type=F32,
                )

        if step is not None:
            logits = scores(0)
        for c in range(HOT_CAP):
            if previous is not None:
                values(c)
            if step is None:
                continue
            for i in range(2 * page // 16):
                j = (2 * c * page + i * 16) // page
                weight = weights_of(logits[i * 16 : (i + 1) * 16]) * allowed[j : j + 1]
                sums = sums + weight[:8] + weight[8:]
                wt[slot, pl.ds(2 * c * page + i * 16, 16), :] = weight.astype(BF16)
            if c + 1 < HOT_CAP:
                logits = scores(c + 1)
        if step is not None:
            res[step, pl.ds(hd, 16), :] = split_sum(jnp.sum(sums, axis=0, keepdims=True), rows)
        if previous is not None:
            for h in range(kvh):
                res[previous, pl.ds(0, hd), pl.ds(h * half, half)] = parts[h].astype(BF16)

    def page_of(place):
        return jnp.maximum(up_s[0, seq_at(place)] - HOT_CAP, 0)

    def own_scores(first, last):
        def some(g, carry):
            seq_of = lax.broadcasted_iota(I32, (page, rows), 1) % seqs
            tile = own_t[...]
            for i in range(0, 16, 2):
                pages = [page_of(g * 16 + i + j) for j in range(2)]
                keys = jnp.concatenate(
                    [jnp.concatenate([kbuf[u, h] for h in range(kvh)], axis=1) for u in pages], axis=0
                )
                logits = jnp.dot(keys, qbd[0], preferred_element_type=F32)
                for j in range(2):
                    tile = jnp.where(seq_of == g * 16 + i + j, logits[j * page : (j + 1) * page], tile)
            own_t[...] = tile
            return carry

        lax.fori_loop(first, last, some, 0)

    def own_weights():
        token = lax.broadcasted_iota(I32, (page, rows), 0).astype(F32)
        weight = jnp.where(token < lrow[pl.ds(0, 1), :], weights_of(own_t[...]), 0.0)
        own_t[pl.ds(0, 8), :] = jnp.broadcast_to(jnp.sum(weight, axis=0, keepdims=True), (8, rows))
        own_w[...] = weight.T

    def own_values():
        local[8].wait()

        def some(n, carry):
            row = lax.broadcasted_iota(I32, (8 * heads, page), 0) % 8
            for m in range(4):
                g = n * 4 + m
                weight = jnp.concatenate([own_w[pl.ds(h * seqs + g * 8, 8), :] for h in range(heads)], axis=0)
                left, right = [], []
                for i in range(8):
                    u = page_of(g * 8 + i)
                    left.append(jnp.where(row == i, weight, 0.0).astype(BF16))
                    right.append(jnp.concatenate([vbuf[u, h] for h in range(kvh)], axis=1))
                part = jnp.dot(
                    jnp.concatenate(left, axis=1), jnp.concatenate(right, axis=0), preferred_element_type=F32
                )
                for h in range(heads):
                    own_o[pl.ds(h * seqs + g * 8, 8), :] = part[h * 8 : (h + 1) * 8]
            return carry

        lax.fori_loop(0, seqs // 32, some, 0)

    set_queries(A0)
    own_t[...] = jnp.zeros_like(own_t)
    local[7].wait()
    own_scores(0, seqs // 32)
    pl.semaphore_wait(far_sem, 1)
    for step in (B3, B1, B2):
        gathers[step].start()
    kv_copies[0].wait_recv()

    def arrive(step, steps):
        for k in steps:
            @pl.when(step == k)
            def _():
                gathers[k].wait_recv()

    def send_back(step, steps):
        for k in steps:
            @pl.when(step == k)
            def _():
                returns[k].start()

    def two_steps(n, carry):
        step = 2 * n + 1
        arrive(step, (1, 3, 5))
        shared_block(step, 1, step - 1)
        send_back(step - 1, (0, 2, 4))
        arrive(step + 1, (2, 4, 6))
        shared_block(step + 1, 0, step)
        send_back(step, (1, 3, 5))
        return carry

    gathers[0].wait_recv()
    shared_block(0, 0, None)
    kv_copies[1].wait_recv()
    transpose_values(HOT_CAP)
    lax.fori_loop(0, 3, two_steps, 0)
    shared_block(None, 1, 6)
    returns[6].start()
    shared_block(7, 1, None)
    shared_block(None, 0, 7)
    own_scores(seqs // 32, seqs // 16)
    own_weights()
    own_values()

    def summed(pieces):
        return sum(piece[...].astype(F32) for piece in pieces)

    own_num = [own_o[pl.ds(h * half, half), pl.ds(h * hd, hd)].T for h in range(kvh)]
    for copy in arrivals.values():
        copy.wait_recv()
    whole = summed([res.at[A0], *(ra.at[k] for k in arrivals)])
    total = jnp.sum(whole[hd:], axis=0, keepdims=True) + own_t[pl.ds(0, 1), :]
    for h in range(kvh):
        lanes = slice(h * half, (h + 1) * half)
        attended = ((whole[:hd, lanes] + own_num[h]) / total[:, lanes]).T.astype(BF16)
        for g in range(half // seqs):
            head = h * (half // seqs) + g
            att[:, pl.ds(head * hd, hd)] = attended[g * seqs : (g + 1) * seqs]

    local[9].wait()
    block = seqs // NZ
    width = w_v.shape[1] // CHUNKS
    relayed, plain, joined, across = {}, {}, {}, {}
    order = [k // 2 + (k % 2) * (CHUNKS // 2) for k in range(CHUNKS)]
    pl.semaphore_wait(diag_sem, 2)
    def piece_of(k):
        return jnp.dot(att[...], w_v[:, pl.ds(k * width, width)], preferred_element_type=F32).astype(BF16)

    piece = piece_of(order[0])
    for n, k in enumerate(order):
        via, other = (1, 3) if k < CHUNKS // 2 else (3, 1)
        cols = pl.ds(k * width, width)
        later = piece_of(order[n + 1]) if n + 1 < CHUNKS else None
        for i in range(NZ):
            for j in range(2):
                pz[i, j, :, cols] = piece[i * block + j * 8 : i * block + j * 8 + 8]
        piece = later

        def to_sum(src, dx, dz, n):
            slot = 4 if dz == 0 else 2 * dx + dz // 2
            return remote(src, zr.at[slot, :, cols], z_send.at[n], z_recv.at[CHUNKS + k], head_at(dx, dz))

        relayed[k] = remote(pz.at[(z + 2) % NZ, :, :, cols], zt.at[:, :, cols], z_send.at[0], z_recv.at[k], head_at(0, via))
        plain[k] = [to_sum(pz.at[(z + other) % NZ, (xl + dx) % 2, :, cols], dx, other, 1) for dx in range(2)]
        joined[k] = [to_sum(zj.at[(xl + dx) % 2, :, cols], dx, via, 2) for dx in range(2)]
        across[k] = [to_sum(pz.at[z, 1 - xl, :, cols], 1, 0, 3)]
        relayed[k].start()
    for k in order:
        for copy in (*plain[k], *across[k]):
            copy.start()
    for k in order:
        via = 1 if k < CHUNKS // 2 else 3
        cols = pl.ds(k * width, width)
        relayed[k].wait_recv()
        for j in range(2):
            zj[j, :, cols] = (pz[(z + via) % NZ, j, :, cols].astype(F32) + zt[j, :, cols].astype(F32)).astype(BF16)
        for copy in joined[k]:
            copy.start()
    square = jnp.zeros((block // 2, 1), F32)
    for k in order:
        cols = pl.ds(k * width, width)
        settle(zr.at[:, :, cols], z_recv.at[CHUNKS + k])
        projected = pz[z, xl, :, cols].astype(F32)
        for i in range(5):
            projected = projected + zr[i, :, cols].astype(F32)
        near_sum[:, cols] = projected
        square = square + jnp.sum(projected * projected, axis=1, keepdims=True)
    out_ref[...] = near_sum[...] / jnp.sqrt(square / w_v.shape[1] + epsilon)

    settle(hk.at[pl.ds(0, 2 * HOT_CAP)], kv_send)
    settle(qt.at[pl.ds(0, len(gathers))], ag_send)
    settle(ra, rs_send)
    for n in range(3):
        settle(zt, z_send.at[n])
    settle(zr.at[0], z_send.at[3])


def layer(queries, keys, values, hot_pages, hot_used, user_pages, lengths, o_weight):
    seqs, heads, hd = queries.shape
    pages, kvh, page, _ = keys.shape
    rows = seqs * heads
    width = o_weight.shape[1]
    vmem = pltpu.VMEM
    return pl.pallas_call(
        layer_kernel,
        out_shape=pltpu.VMEM((seqs // 8, width), F32),
        in_specs=[pl.BlockSpec(memory_space=pl.ANY)] * 8,
        out_specs=pl.BlockSpec(memory_space=pltpu.VMEM),
        scratch_shapes=[
            vmem((rows, hd), BF16),
            vmem((1, hot_pages.shape[0]), I32),
            vmem((hot_used.shape[0] // 128, 128), I32),
            vmem((1, seqs), I32),
            pltpu.SMEM((1, seqs), I32),
            vmem((pages - HOT_CAP, kvh, page, hd), BF16),
            vmem((pages - HOT_CAP, kvh, page, hd), BF16),
            vmem((2 * HOT_CAP, kvh, page, hd), BF16),
            vmem((2 * HOT_CAP, kvh, page, hd), BF16),
            vmem((kvh, hd, 2 * HOT_CAP * page), BF16),
            vmem((8, hd, rows), BF16),
            vmem((1, kvh * hd, rows), BF16),
            vmem((8, rows), F32),
            vmem((8, rows), F32),
            vmem((2 * HOT_CAP, 128), F32),
            vmem((2, 2 * HOT_CAP * page, rows), BF16),
            vmem((8, hd + 16, rows), BF16),
            vmem((7, hd + 16, rows), BF16),
            vmem((page, rows), F32),
            vmem((rows, page), F32),
            vmem((rows, kvh * hd), F32),
            vmem(o_weight.shape, BF16),
            vmem((seqs, heads * hd), BF16),
            vmem((NZ, 2, 8, width), BF16),
            vmem((2, 8, width), BF16),
            vmem((2, 8, width), BF16),
            vmem((5, 8, width), BF16),
            vmem((seqs // 8, width), F32),
            pltpu.SemaphoreType.DMA((10,)),
            pltpu.SemaphoreType.DMA((4,)),
            pltpu.SemaphoreType.DMA((2 * CHUNKS,)),
            pltpu.SemaphoreType.DMA,
            pltpu.SemaphoreType.DMA((2,)),
            pltpu.SemaphoreType.DMA,
            pltpu.SemaphoreType.DMA((7,)),
            pltpu.SemaphoreType.DMA,
            pltpu.SemaphoreType.DMA((7,)),
            pltpu.SemaphoreType.REGULAR,
            pltpu.SemaphoreType.REGULAR,
        ],
        compiler_params=pltpu.CompilerParams(
            collective_id=0, has_side_effects=True, vmem_limit_bytes=64_500_000
        ),
        name="layer",
    )(
        queries.reshape(rows, hd),
        keys,
        values,
        hot_pages.reshape(1, -1),
        hot_used.reshape(-1, 128),
        user_pages.reshape(1, -1),
        lengths.reshape(1, -1),
        o_weight,
    )


def per_device(
    queries, keys, values, hot_pages, hot_used, user_pages, lengths, o_weight, residual, norm_gain
):
    normed = layer(queries, keys, values, hot_pages, hot_used, user_pages, lengths, o_weight)
    return (residual.astype(F32) + normed * norm_gain[None, :]).astype(BF16)


def solution(mesh):
    in_specs = (
        P("pages", "heads", None),
        P("pages", "heads", None, None),
        P("pages", "heads", None, None),
        P(),
        P(),
        P("pages", None),
        P("pages"),
        P("heads", None),
        P(("pages", "heads"), None),
        P(),
    )
    out_specs = P(("pages", "heads"), None)
    return jax.shard_map(
        per_device, mesh=mesh, in_specs=in_specs, out_specs=out_specs, check_vma=False
    )
```

```python
import functools
import math

import jax
import jax.numpy as jnp
from jax import lax
from jax.experimental import pallas as pl
from jax.experimental.pallas import tpu as pltpu
from jax.sharding import PartitionSpec as P

HOT_CAP = 8
soft_cap = 50.0
score_scale = 1.0 / 12.0
epsilon = 1e-06
NY = 4
NZ = 4
CHUNKS = 6
F32, BF16, I32 = jnp.float32, jnp.bfloat16, jnp.int32
MESH = pl.DeviceIdType.MESH

A3, B0, A1, A2, B2, B1, B3, A0 = range(8)
OWNER = {A3: (3, 0), A1: (1, 0), A2: (2, 0), B0: (0, 1), B3: (3, 1), B1: (1, 1), B2: (2, 1), A0: (0, 0)}


def weights_of(logits):
    return jnp.exp2(jnp.tanh(logits * (score_scale / soft_cap)) * (soft_cap * math.log2(math.e)))


def split_sum(totals, rows):
    high = totals.astype(BF16).astype(F32)
    row = lax.broadcasted_iota(I32, (16, rows), 0)
    return jnp.where(row == 0, high, jnp.where(row == 1, totals - high, 0.0)).astype(BF16)


def layer_kernel(
    q_hbm, k_hbm, v_hbm, hot_hbm, used_hbm, up_hbm, len_hbm, w_hbm, out_ref,
    q_v, hot_v, used_v, len_v, up_s, kbuf, vbuf, hk, hv, vt, qt, qbd, urow, lrow, pos,
    wt, res, ra, own_t, own_w, own_o,
    w_v, att, pz, zt, zj, zr, near_sum,
    in_sem, z_send, z_recv, kv_send, kv_recv, ag_send, ag_recv, rs_send, rs_recv, far_sem, diag_sem,
):
    seqs = len_v.shape[1]
    kvh, page, hd = hk.shape[1:]
    rows = q_v.shape[0]
    half = rows // kvh
    me = lax.axis_index("pages")
    y, xh, core = me // 4, (me // 2) % 2, me % 2

    member = lax.axis_index("heads")
    xl, z = member // NZ, member % NZ

    def head_at(dx, dz):
        return {"heads": ((xl + dx) % 2) * NZ + (z + dz) % NZ}

    def seq_at(place):
        return ((place // 8) % 2) * (seqs // 2) + (place // 16) * 8 + place % 8

    def at(dy, dx=0, dc=0):
        return {"pages": ((y + dy) % NY) * 4 + ((xh + dx) % 2) * 2 + (core + dc) % 2}

    def remote(src, dst, send, recv, target):
        return pltpu.make_async_remote_copy(
            src_ref=src, dst_ref=dst, send_sem=send, recv_sem=recv, device_id=target, device_id_type=MESH
        )

    own = pl.ds(HOT_CAP, k_hbm.shape[0] - HOT_CAP)
    hot = pl.ds(0, HOT_CAP)
    def settle(like, semaphore):
        pltpu.make_async_copy(like, like, semaphore).wait()

    local = [
        pltpu.make_async_copy(q_hbm, q_v, in_sem.at[0]),
        pltpu.make_async_copy(hot_hbm, hot_v, in_sem.at[1]),
        pltpu.make_async_copy(used_hbm, used_v, in_sem.at[2]),
        pltpu.make_async_copy(len_hbm, len_v, in_sem.at[3]),
        pltpu.make_async_copy(up_hbm, up_s, in_sem.at[4]),
        pltpu.make_async_copy(k_hbm.at[hot], hk.at[hot], in_sem.at[5]),
        pltpu.make_async_copy(v_hbm.at[hot], hv.at[hot], in_sem.at[6]),
        pltpu.make_async_copy(k_hbm.at[own], kbuf, in_sem.at[7]),
        pltpu.make_async_copy(v_hbm.at[own], vbuf, in_sem.at[8]),
        pltpu.make_async_copy(w_hbm, w_v, in_sem.at[9]),
    ]
    for copy in local[:8]:
        copy.start()

    barrier = pltpu.get_barrier_semaphore()
    peers = [at(1), at(2), at(3), at(0, 1), at(0, 0, 1)]
    peers += [head_at(0, 1), head_at(0, 2), head_at(0, 3), head_at(1, 0)]
    for peer in peers:
        pl.semaphore_signal(barrier, inc=1, device_id=peer, device_id_type=MESH)

    r = lax.broadcasted_iota(I32, (rows, rows), 0)
    col = lax.broadcasted_iota(I32, (rows, rows), 1)
    heads = rows // seqs
    perm = jnp.where(col == seq_at(r % seqs) * heads + r // seqs, 1.0, 0.0).astype(BF16)
    local[0].wait()
    q_rows = jnp.dot(perm, q_v[...], preferred_element_type=F32)
    qt[A0] = q_rows.T.astype(BF16)

    pl.semaphore_wait(barrier, len(peers))

    far = pl.ds(HOT_CAP, HOT_CAP)
    kv_copies = [
        remote(hk.at[hot], hk.at[far], kv_send, kv_recv.at[0], at(0, 0, 1)),
        remote(hv.at[hot], hv.at[far], kv_send, kv_recv.at[1], at(0, 0, 1)),
    ]
    gathers, returns = {}, {}
    for step, (dy, dx) in OWNER.items():
        if step == A0:
            continue
        back = next(k for k, at_ in OWNER.items() if at_ == ((NY - dy) % NY, dx))
        gathers[step] = remote(qt.at[A0], qt.at[step], ag_send, ag_recv.at[step], at((NY - dy) % NY, dx))
        returns[step] = remote(res.at[step], ra.at[back], rs_send, rs_recv, at(dy, dx))
    pl.semaphore_signal(far_sem, inc=1, device_id=at(0, 1), device_id_type=MESH)
    for dz in (1, 3):
        pl.semaphore_signal(diag_sem, inc=1, device_id=head_at(0, dz), device_id_type=MESH)
    for step in (B0, A3, A1, A2):
        gathers[step].start()
    local[5].wait()
    local[6].wait()
    kv_copies[0].start()
    local[8].start()
    local[9].start()

    for copy in local[1:5]:
        copy.wait()
    lane = lax.broadcasted_iota(I32, (2 * seqs, rows), 0)
    pick = seq_at(lax.broadcasted_iota(I32, (2 * seqs, rows), 1) % seqs)
    spread = jnp.where(lane == core * seqs + pick, 1.0, 0.0).astype(BF16)
    used = jnp.dot(used_v[...].astype(F32).astype(BF16), spread, preferred_element_type=F32)
    own_t[pl.ds(0, 8), :] = used
    for step, (dy, dx) in OWNER.items():
        chip = ((y + dy) % NY) * 2 + (xh + dx) % 2
        urow[pl.ds(step, 1), :] = own_t[pl.ds(chip, 1), :]
    lane = lax.broadcasted_iota(I32, (seqs, rows), 0)
    pick = seq_at(lax.broadcasted_iota(I32, (seqs, rows), 1) % seqs)
    spread = jnp.where(lane == pick, 1.0, 0.0).astype(BF16)
    lens = jnp.broadcast_to(len_v[...].astype(F32), (8, seqs)).astype(BF16)
    lrow[...] = jnp.dot(lens, spread, preferred_element_type=F32)
    hot_n = hot_v.shape[1]
    cand = lax.broadcasted_iota(I32, (2 * HOT_CAP, hot_n), 0)
    group = jnp.where(cand < HOT_CAP, me, at(0, 0, 1)["pages"])
    match = hot_v[...] == group * k_hbm.shape[0] + cand % HOT_CAP
    order = lax.broadcasted_iota(I32, (2 * HOT_CAP, hot_n), 1).astype(F32)
    pos[...] = jnp.broadcast_to(
        jnp.min(jnp.where(match, order, 1e9), axis=1, keepdims=True), pos.shape
    )

    qbd[...] = jnp.zeros_like(qbd)

    def set_queries(step):
        qbd[0, pl.ds(0, hd), pl.ds(0, half)] = qt[step, :, pl.ds(0, half)]
        qbd[0, pl.ds(hd, hd), pl.ds(half, half)] = qt[step, :, pl.ds(half, half)]

    def transpose_values(first):
        for j in range(first, first + HOT_CAP):
            for h in range(kvh):
                vt[h, :, pl.ds(j * page, page)] = hv[j, h].T

    transpose_values(0)

    def shared_block(step, slot, previous):
        if step is not None:
            set_queries(step)
            allowed = jnp.where(urow[pl.ds(step, 1), :] > pos[:, pl.ds(0, 1)], 1.0, 0.0)
            sums = jnp.zeros((8, rows), F32)
        parts = [jnp.zeros((hd, half), F32) for _ in range(kvh)]

        def scores(c):
            keys = jnp.concatenate(
                [hk[pl.ds(2 * c, 2), h].reshape(2 * page, hd) for h in range(kvh)], axis=1
            )
            return jnp.dot(keys, qbd[0], preferred_element_type=F32)

        def values(c):
            for h in range(kvh):
                parts[h] = parts[h] + jnp.dot(
                    vt[h, :, pl.ds(2 * c * page, 2 * page)],
                    wt[1 - slot, pl.ds(2 * c * page, 2 * page), pl.ds(h * half, half)],
                    preferred_element_type=F32,
                )

        if step is not None:
            logits = scores(0)
        for c in range(HOT_CAP):
            if previous is not None:
                values(c)
            if step is None:
                continue
            for i in range(2 * page // 16):
                j = (2 * c * page + i * 16) // page
                weight = weights_of(logits[i * 16 : (i + 1) * 16]) * allowed[j : j + 1]
                sums = sums + weight[:8] + weight[8:]
                wt[slot, pl.ds(2 * c * page + i * 16, 16), :] = weight.astype(BF16)
            if c + 1 < HOT_CAP:
                logits = scores(c + 1)
        if step is not None:
            res[step, pl.ds(hd, 16), :] = split_sum(jnp.sum(sums, axis=0, keepdims=True), rows)
        if previous is not None:
            for h in range(kvh):
                res[previous, pl.ds(0, hd), pl.ds(h * half, half)] = parts[h].astype(BF16)

    def page_of(place):
        return jnp.maximum(up_s[0, seq_at(place)] - HOT_CAP, 0)

    def own_scores(first, last):
        def some(g, carry):
            seq_of = lax.broadcasted_iota(I32, (page, rows), 1) % seqs
            tile = own_t[...]
            for i in range(0, 16, 2):
                pages = [page_of(g * 16 + i + j) for j in range(2)]
                keys = jnp.concatenate(
                    [jnp.concatenate([kbuf[u, h] for h in range(kvh)], axis=1) for u in pages], axis=0
                )
                logits = jnp.dot(keys, qbd[0], preferred_element_type=F32)
                for j in range(2):
                    tile = jnp.where(seq_of == g * 16 + i + j, logits[j * page : (j + 1) * page], tile)
            own_t[...] = tile
            return carry

        lax.fori_loop(first, last, some, 0)

    def own_weights():
        token = lax.broadcasted_iota(I32, (page, rows), 0).astype(F32)
        weight = jnp.where(token < lrow[pl.ds(0, 1), :], weights_of(own_t[...]), 0.0)
        own_t[pl.ds(0, 8), :] = jnp.broadcast_to(jnp.sum(weight, axis=0, keepdims=True), (8, rows))
        own_w[...] = weight.T

    def own_values():
        local[8].wait()

        def some(n, carry):
            row = lax.broadcasted_iota(I32, (8 * heads, page), 0) % 8
            for m in range(4):
                g = n * 4 + m
                weight = jnp.concatenate([own_w[pl.ds(h * seqs + g * 8, 8), :] for h in range(heads)], axis=0)
                left, right = [], []
                for i in range(8):
                    u = page_of(g * 8 + i)
                    left.append(jnp.where(row == i, weight, 0.0).astype(BF16))
                    right.append(jnp.concatenate([vbuf[u, h] for h in range(kvh)], axis=1))
                part = jnp.dot(
                    jnp.concatenate(left, axis=1), jnp.concatenate(right, axis=0), preferred_element_type=F32
                )
                for h in range(heads):
                    own_o[pl.ds(h * seqs + g * 8, 8), :] = part[h * 8 : (h + 1) * 8]
            return carry

        lax.fori_loop(0, seqs // 32, some, 0)

    set_queries(A0)
    own_t[...] = jnp.zeros_like(own_t)
    local[7].wait()
    own_scores(0, seqs // 32)
    pl.semaphore_wait(far_sem, 1)
    for step in (B2, B1, B3):
        gathers[step].start()
    kv_copies[1].start()
    kv_copies[0].wait_recv()

    def arrive(step, steps):
        for k in steps:
            @pl.when(step == k)
            def _():
                gathers[k].wait_recv()

    def send_back(step, steps):
        for k in steps:
            @pl.when(step == k)
            def _():
                returns[k].start()

    def two_steps(n, carry):
        step = 2 * n + 1
        arrive(step, (1, 3, 5))
        shared_block(step, 1, step - 1)
        send_back(step - 1, (0, 2, 4))
        arrive(step + 1, (2, 4, 6))
        shared_block(step + 1, 0, step)
        send_back(step, (1, 3, 5))
        return carry

    gathers[0].wait_recv()
    shared_block(0, 0, None)
    kv_copies[1].wait_recv()
    transpose_values(HOT_CAP)
    lax.fori_loop(0, 3, two_steps, 0)
    shared_block(None, 1, 6)
    returns[6].start()
    shared_block(7, 1, None)
    shared_block(None, 0, 7)
    own_scores(seqs // 32, seqs // 16)
    own_weights()
    own_values()

    def summed(pieces):
        return sum(piece[...].astype(F32) for piece in pieces)

    own_num = [own_o[pl.ds(h * half, half), pl.ds(h * hd, hd)].T for h in range(kvh)]
    settle(ra, rs_recv)
    whole = summed([res.at[A0], *(ra.at[k] for k in returns)])
    total = jnp.sum(whole[hd:], axis=0, keepdims=True) + own_t[pl.ds(0, 1), :]
    for h in range(kvh):
        lanes = slice(h * half, (h + 1) * half)
        attended = ((whole[:hd, lanes] + own_num[h]) / total[:, lanes]).T.astype(BF16)
        for g in range(half // seqs):
            head = h * (half // seqs) + g
            att[:, pl.ds(head * hd, hd)] = attended[g * seqs : (g + 1) * seqs]

    local[9].wait()
    block = seqs // NZ
    width = w_v.shape[1] // CHUNKS
    relayed, plain, joined, across = {}, {}, {}, {}
    order = [k // 2 + (k % 2) * (CHUNKS // 2) for k in range(CHUNKS)]
    pl.semaphore_wait(diag_sem, 2)
    def piece_of(k):
        return jnp.dot(att[...], w_v[:, pl.ds(k * width, width)], preferred_element_type=F32).astype(BF16)

    piece = piece_of(order[0])
    for n, k in enumerate(order):
        via, other = (1, 3) if k < CHUNKS // 2 else (3, 1)
        cols = pl.ds(k * width, width)
        later = piece_of(order[n + 1]) if n + 1 < CHUNKS else None
        for i in range(NZ):
            for j in range(2):
                pz[i, j, :, cols] = piece[i * block + j * 8 : i * block + j * 8 + 8]
        piece = later

        def to_sum(src, dx, dz, n):
            slot = 4 if dz == 0 else 2 * dx + dz // 2
            return remote(src, zr.at[slot, :, cols], z_send.at[n], z_recv.at[CHUNKS + k], head_at(dx, dz))

        relayed[k] = remote(pz.at[(z + 2) % NZ, :, :, cols], zt.at[:, :, cols], z_send.at[0], z_recv.at[k], head_at(0, via))
        plain[k] = [to_sum(pz.at[(z + other) % NZ, (xl + dx) % 2, :, cols], dx, other, 1) for dx in range(2)]
        joined[k] = [to_sum(zj.at[(xl + dx) % 2, :, cols], dx, via, 2) for dx in range(2)]
        across[k] = [to_sum(pz.at[z, 1 - xl, :, cols], 1, 0, 3)]
        relayed[k].start()
    for k in order:
        for copy in (*plain[k], *across[k]):
            copy.start()
    for k in order:
        via = 1 if k < CHUNKS // 2 else 3
        cols = pl.ds(k * width, width)
        relayed[k].wait_recv()
        for j in range(2):
            zj[j, :, cols] = (pz[(z + via) % NZ, j, :, cols].astype(F32) + zt[j, :, cols].astype(F32)).astype(BF16)
        for copy in joined[k]:
            copy.start()
    square = jnp.zeros((block // 2, 1), F32)
    for k in order:
        cols = pl.ds(k * width, width)
        settle(zr.at[:, :, cols], z_recv.at[CHUNKS + k])
        projected = pz[z, xl, :, cols].astype(F32)
        for i in range(5):
            projected = projected + zr[i, :, cols].astype(F32)
        near_sum[:, cols] = projected
        square = square + jnp.sum(projected * projected, axis=1, keepdims=True)
    out_ref[...] = near_sum[...] / jnp.sqrt(square / w_v.shape[1] + epsilon)

    settle(hk.at[pl.ds(0, 2 * HOT_CAP)], kv_send)
    settle(qt.at[pl.ds(0, len(gathers))], ag_send)
    settle(ra, rs_send)
    for n in range(3):
        settle(zt, z_send.at[n])
    settle(zr.at[0], z_send.at[3])


def layer(queries, keys, values, hot_pages, hot_used, user_pages, lengths, o_weight):
    seqs, heads, hd = queries.shape
    pages, kvh, page, _ = keys.shape
    rows = seqs * heads
    width = o_weight.shape[1]
    vmem = pltpu.VMEM
    return pl.pallas_call(
        layer_kernel,
        out_shape=pltpu.VMEM((seqs // 8, width), F32),
        in_specs=[pl.BlockSpec(memory_space=pl.ANY)] * 8,
        out_specs=pl.BlockSpec(memory_space=pltpu.VMEM),
        scratch_shapes=[
            vmem((rows, hd), BF16),
            vmem((1, hot_pages.shape[0]), I32),
            vmem((hot_used.shape[0] // 128, 128), I32),
            vmem((1, seqs), I32),
            pltpu.SMEM((1, seqs), I32),
            vmem((pages - HOT_CAP, kvh, page, hd), BF16),
            vmem((pages - HOT_CAP, kvh, page, hd), BF16),
            vmem((2 * HOT_CAP, kvh, page, hd), BF16),
            vmem((2 * HOT_CAP, kvh, page, hd), BF16),
            vmem((kvh, hd, 2 * HOT_CAP * page), BF16),
            vmem((8, hd, rows), BF16),
            vmem((1, kvh * hd, rows), BF16),
            vmem((8, rows), F32),
            vmem((8, rows), F32),
            vmem((2 * HOT_CAP, 128), F32),
            vmem((2, 2 * HOT_CAP * page, rows), BF16),
            vmem((8, hd + 16, rows), BF16),
            vmem((7, hd + 16, rows), BF16),
            vmem((page, rows), F32),
            vmem((rows, page), F32),
            vmem((rows, kvh * hd), F32),
            vmem(o_weight.shape, BF16),
            vmem((seqs, heads * hd), BF16),
            vmem((NZ, 2, 8, width), BF16),
            vmem((2, 8, width), BF16),
            vmem((2, 8, width), BF16),
            vmem((5, 8, width), BF16),
            vmem((seqs // 8, width), F32),
            pltpu.SemaphoreType.DMA((10,)),
            pltpu.SemaphoreType.DMA((4,)),
            pltpu.SemaphoreType.DMA((2 * CHUNKS,)),
            pltpu.SemaphoreType.DMA,
            pltpu.SemaphoreType.DMA((2,)),
            pltpu.SemaphoreType.DMA,
            pltpu.SemaphoreType.DMA((7,)),
            pltpu.SemaphoreType.DMA,
            pltpu.SemaphoreType.DMA,
            pltpu.SemaphoreType.REGULAR,
            pltpu.SemaphoreType.REGULAR,
        ],
        compiler_params=pltpu.CompilerParams(
            collective_id=0, has_side_effects=True, vmem_limit_bytes=64_500_000
        ),
        name="layer",
    )(
        queries.reshape(rows, hd),
        keys,
        values,
        hot_pages.reshape(1, -1),
        hot_used.reshape(-1, 128),
        user_pages.reshape(1, -1),
        lengths.reshape(1, -1),
        o_weight,
    )


def per_device(
    queries, keys, values, hot_pages, hot_used, user_pages, lengths, o_weight, residual, norm_gain
):
    normed = layer(queries, keys, values, hot_pages, hot_used, user_pages, lengths, o_weight)
    return (residual.astype(F32) + normed * norm_gain[None, :]).astype(BF16)


def solution(mesh):
    in_specs = (
        P("pages", "heads", None),
        P("pages", "heads", None, None),
        P("pages", "heads", None, None),
        P(),
        P(),
        P("pages", None),
        P("pages"),
        P("heads", None),
        P(("pages", "heads"), None),
        P(),
    )
    out_specs = P(("pages", "heads"), None)
    return jax.shard_map(
        per_device, mesh=mesh, in_specs=in_specs, out_specs=out_specs, check_vma=False
    )
```

```python
import functools
import math

import jax
import jax.numpy as jnp
from jax import lax
from jax.experimental import pallas as pl
from jax.experimental.pallas import tpu as pltpu
from jax.sharding import PartitionSpec as P

HOT_CAP = 8
soft_cap = 50.0
score_scale = 1.0 / 12.0
epsilon = 1e-06
NY = 4
NZ = 4
CHUNKS = 6
F32, BF16, I32 = jnp.float32, jnp.bfloat16, jnp.int32
MESH = pl.DeviceIdType.MESH

A3, B0, A1, A2, B2, B1, B3, A0 = range(8)
OWNER = {A3: (3, 0), A1: (1, 0), A2: (2, 0), B0: (0, 1), B3: (3, 1), B1: (1, 1), B2: (2, 1), A0: (0, 0)}


def weights_of(logits):
    return jnp.exp2(jnp.tanh(logits * (score_scale / soft_cap)) * (soft_cap * math.log2(math.e)))


def layer_kernel(
    q_hbm, k_hbm, v_hbm, hot_hbm, used_hbm, up_hbm, len_hbm, w_hbm, out_ref,
    q_v, hot_v, used_v, len_v, up_s, kbuf, vbuf, hk, hv, vt, qt, qbd, urow, lrow, pos,
    wt, res, ra, tot, tot_ra, own_t, own_w, own_o,
    w_v, att, pz, zt, zj, zr, near_sum,
    in_sem, z_send, z_recv, kv_send, kv_recv, ag_send, ag_recv, rs_send, rs_recv, tot_send, tot_recv, far_sem, diag_sem,
):
    seqs = len_v.shape[1]
    kvh, page, hd = hk.shape[1:]
    rows = q_v.shape[0]
    half = rows // kvh
    me = lax.axis_index("pages")
    y, xh, core = me // 4, (me // 2) % 2, me % 2

    member = lax.axis_index("heads")
    xl, z = member // NZ, member % NZ

    def head_at(dx, dz):
        return {"heads": ((xl + dx) % 2) * NZ + (z + dz) % NZ}

    def seq_at(place):
        return ((place // 8) % 2) * (seqs // 2) + (place // 16) * 8 + place % 8

    def at(dy, dx=0, dc=0):
        return {"pages": ((y + dy) % NY) * 4 + ((xh + dx) % 2) * 2 + (core + dc) % 2}

    def remote(src, dst, send, recv, target):
        return pltpu.make_async_remote_copy(
            src_ref=src, dst_ref=dst, send_sem=send, recv_sem=recv, device_id=target, device_id_type=MESH
        )

    own = pl.ds(HOT_CAP, k_hbm.shape[0] - HOT_CAP)
    hot = pl.ds(0, HOT_CAP)
    def settle(like, semaphore):
        pltpu.make_async_copy(like, like, semaphore).wait()

    local = [
        pltpu.make_async_copy(q_hbm, q_v, in_sem.at[0]),
        pltpu.make_async_copy(hot_hbm, hot_v, in_sem.at[1]),
        pltpu.make_async_copy(used_hbm, used_v, in_sem.at[2]),
        pltpu.make_async_copy(len_hbm, len_v, in_sem.at[3]),
        pltpu.make_async_copy(up_hbm, up_s, in_sem.at[4]),
        pltpu.make_async_copy(k_hbm.at[hot], hk.at[hot], in_sem.at[5]),
        pltpu.make_async_copy(v_hbm.at[hot], hv.at[hot], in_sem.at[6]),
        pltpu.make_async_copy(k_hbm.at[own], kbuf, in_sem.at[7]),
        pltpu.make_async_copy(v_hbm.at[own], vbuf, in_sem.at[8]),
        pltpu.make_async_copy(w_hbm, w_v, in_sem.at[9]),
    ]
    for copy in local[:8]:
        copy.start()

    barrier = pltpu.get_barrier_semaphore()
    peers = [at(1), at(2), at(3), at(0, 1), at(0, 0, 1)]
    peers += [head_at(0, 1), head_at(0, 3), head_at(1, 0)]
    for peer in peers:
        pl.semaphore_signal(barrier, inc=1, device_id=peer, device_id_type=MESH)

    r = lax.broadcasted_iota(I32, (rows, rows), 0)
    col = lax.broadcasted_iota(I32, (rows, rows), 1)
    heads = rows // seqs
    perm = jnp.where(col == seq_at(r % seqs) * heads + r // seqs, 1.0, 0.0).astype(BF16)
    local[0].wait()
    q_rows = jnp.dot(perm, q_v[...], preferred_element_type=F32)
    qt[A0] = q_rows.T.astype(BF16)

    pl.semaphore_wait(barrier, len(peers))

    far = pl.ds(HOT_CAP, HOT_CAP)
    kv_copies = [
        remote(hk.at[hot], hk.at[far], kv_send, kv_recv.at[0], at(0, 0, 1)),
        remote(hv.at[hot], hv.at[far], kv_send, kv_recv.at[1], at(0, 0, 1)),
    ]
    gathers, returns = {}, {}
    for step, (dy, dx) in OWNER.items():
        if step == A0:
            continue
        back = next(k for k, at_ in OWNER.items() if at_ == ((NY - dy) % NY, dx))
        gathers[step] = remote(qt.at[A0], qt.at[step], ag_send, ag_recv.at[step], at((NY - dy) % NY, dx))
        returns[step] = [
            remote(res.at[step], ra.at[back], rs_send, rs_recv, at(dy, dx)),
            remote(tot.at[step], tot_ra.at[back], tot_send, tot_recv, at(dy, dx)),
        ]
    pl.semaphore_signal(far_sem, inc=1, device_id=at(0, 1), device_id_type=MESH)
    for dz in (1, 3):
        pl.semaphore_signal(diag_sem, inc=1, device_id=head_at(0, dz), device_id_type=MESH)
    for step in (B0, A3, A1, A2):
        gathers[step].start()
    local[5].wait()
    local[6].wait()
    kv_copies[0].start()
    local[8].start()
    local[9].start()

    for copy in local[1:5]:
        copy.wait()
    lane = lax.broadcasted_iota(I32, (2 * seqs, rows), 0)
    pick = seq_at(lax.broadcasted_iota(I32, (2 * seqs, rows), 1) % seqs)
    spread = jnp.where(lane == core * seqs + pick, 1.0, 0.0).astype(BF16)
    used = jnp.dot(used_v[...].astype(F32).astype(BF16), spread, preferred_element_type=F32)
    own_t[pl.ds(0, 8), :] = used
    for step, (dy, dx) in OWNER.items():
        chip = ((y + dy) % NY) * 2 + (xh + dx) % 2
        urow[pl.ds(step, 1), :] = own_t[pl.ds(chip, 1), :]
    lane = lax.broadcasted_iota(I32, (seqs, rows), 0)
    pick = seq_at(lax.broadcasted_iota(I32, (seqs, rows), 1) % seqs)
    spread = jnp.where(lane == pick, 1.0, 0.0).astype(BF16)
    lens = jnp.broadcast_to(len_v[...].astype(F32), (8, seqs)).astype(BF16)
    lrow[...] = jnp.dot(lens, spread, preferred_element_type=F32)
    hot_n = hot_v.shape[1]
    cand = lax.broadcasted_iota(I32, (2 * HOT_CAP, hot_n), 0)
    group = jnp.where(cand < HOT_CAP, me, at(0, 0, 1)["pages"])
    match = hot_v[...] == group * k_hbm.shape[0] + cand % HOT_CAP
    order = lax.broadcasted_iota(I32, (2 * HOT_CAP, hot_n), 1).astype(F32)
    pos[...] = jnp.broadcast_to(
        jnp.min(jnp.where(match, order, 1e9), axis=1, keepdims=True), pos.shape
    )

    qbd[...] = jnp.zeros_like(qbd)

    def set_queries(step):
        qbd[0, pl.ds(0, hd), pl.ds(0, half)] = qt[step, :, pl.ds(0, half)]
        qbd[0, pl.ds(hd, hd), pl.ds(half, half)] = qt[step, :, pl.ds(half, half)]

    def transpose_values(first):
        for j in range(first, first + HOT_CAP):
            for h in range(kvh):
                vt[h, :, pl.ds(j * page, page)] = hv[j, h].T

    transpose_values(0)

    def shared_block(step, slot, previous):
        if step is not None:
            set_queries(step)
            allowed = jnp.where(urow[pl.ds(step, 1), :] > pos[:, pl.ds(0, 1)], 1.0, 0.0)
            sums = jnp.zeros((8, rows), F32)
        parts = [jnp.zeros((hd, half), F32) for _ in range(kvh)]

        def scores(c):
            keys = jnp.concatenate(
                [hk[pl.ds(2 * c, 2), h].reshape(2 * page, hd) for h in range(kvh)], axis=1
            )
            return jnp.dot(keys, qbd[0], preferred_element_type=F32)

        def values(c):
            for h in range(kvh):
                parts[h] = parts[h] + jnp.dot(
                    vt[h, :, pl.ds(2 * c * page, 2 * page)],
                    wt[1 - slot, pl.ds(2 * c * page, 2 * page), pl.ds(h * half, half)],
                    preferred_element_type=F32,
                )

        if step is not None:
            logits = scores(0)
        for c in range(HOT_CAP):
            if previous is not None:
                values(c)
            if step is None:
                continue
            for i in range(2 * page // 16):
                j = (2 * c * page + i * 16) // page
                weight = weights_of(logits[i * 16 : (i + 1) * 16]) * allowed[j : j + 1]
                sums = sums + weight[:8] + weight[8:]
                wt[slot, pl.ds(2 * c * page + i * 16, 16), :] = weight.astype(BF16)
            if c + 1 < HOT_CAP:
                logits = scores(c + 1)
        if step is not None:
            tot[step] = jnp.sum(sums, axis=0, keepdims=True)
        if previous is not None:
            for h in range(kvh):
                res[previous, :, pl.ds(h * half, half)] = parts[h].astype(BF16)

    def page_of(place):
        return jnp.maximum(up_s[0, seq_at(place)] - HOT_CAP, 0)

    def own_scores(first, last):
        def some(g, carry):
            seq_of = lax.broadcasted_iota(I32, (page, rows), 1) % seqs
            tile = own_t[...]
            for i in range(0, 16, 2):
                pages = [page_of(g * 16 + i + j) for j in range(2)]
                keys = jnp.concatenate(
                    [jnp.concatenate([kbuf[u, h] for h in range(kvh)], axis=1) for u in pages], axis=0
                )
                logits = jnp.dot(keys, qbd[0], preferred_element_type=F32)
                for j in range(2):
                    tile = jnp.where(seq_of == g * 16 + i + j, logits[j * page : (j + 1) * page], tile)
            own_t[...] = tile
            return carry

        lax.fori_loop(first, last, some, 0)

    def own_weights():
        token = lax.broadcasted_iota(I32, (page, rows), 0).astype(F32)
        weight = jnp.where(token < lrow[pl.ds(0, 1), :], weights_of(own_t[...]), 0.0)
        own_t[pl.ds(0, 8), :] = jnp.broadcast_to(jnp.sum(weight, axis=0, keepdims=True), (8, rows))
        own_w[...] = weight.T

    def own_values():
        local[8].wait()

        def some(n, carry):
            row = lax.broadcasted_iota(I32, (8 * heads, page), 0) % 8
            for m in range(4):
                g = n * 4 + m
                weight = jnp.concatenate([own_w[pl.ds(h * seqs + g * 8, 8), :] for h in range(heads)], axis=0)
                left, right = [], []
                for i in range(8):
                    u = page_of(g * 8 + i)
                    left.append(jnp.where(row == i, weight, 0.0).astype(BF16))
                    right.append(jnp.concatenate([vbuf[u, h] for h in range(kvh)], axis=1))
                part = jnp.dot(
                    jnp.concatenate(left, axis=1), jnp.concatenate(right, axis=0), preferred_element_type=F32
                )
                for h in range(heads):
                    own_o[pl.ds(h * seqs + g * 8, 8), :] = part[h * 8 : (h + 1) * 8]
            return carry

        lax.fori_loop(0, seqs // 32, some, 0)

    set_queries(A0)
    own_t[...] = jnp.zeros_like(own_t)
    local[7].wait()
    own_scores(0, seqs // 32)
    pl.semaphore_wait(far_sem, 1)
    for step in (B2, B1, B3):
        gathers[step].start()
    kv_copies[1].start()
    kv_copies[0].wait_recv()

    def arrive(step, steps):
        for k in steps:
            @pl.when(step == k)
            def _():
                gathers[k].wait_recv()

    def send_back(step, steps):
        for k in steps:
            @pl.when(step == k)
            def _():
                for copy in returns[k]:
                    copy.start()

    def two_steps(n, carry):
        step = 2 * n + 1
        arrive(step, (1, 3, 5))
        shared_block(step, 1, step - 1)
        send_back(step - 1, (0, 2, 4))
        arrive(step + 1, (2, 4, 6))
        shared_block(step + 1, 0, step)
        send_back(step, (1, 3, 5))
        return carry

    gathers[0].wait_recv()
    shared_block(0, 0, None)
    kv_copies[1].wait_recv()
    transpose_values(HOT_CAP)
    lax.fori_loop(0, 3, two_steps, 0)
    shared_block(None, 1, 6)
    for copy in returns[6]:
        copy.start()
    shared_block(7, 1, None)
    shared_block(None, 0, 7)
    own_scores(seqs // 32, seqs // 16)
    own_weights()
    own_values()

    def summed(pieces):
        return sum(piece[...].astype(F32) for piece in pieces)

    own_num = [own_o[pl.ds(h * half, half), pl.ds(h * hd, hd)].T for h in range(kvh)]
    settle(ra, rs_recv)
    settle(tot_ra, tot_recv)
    whole = summed([res.at[A0], *(ra.at[k] for k in returns)])
    total = sum((tot_ra[k] for k in returns), tot[A0]) + own_t[pl.ds(0, 1), :]
    for h in range(kvh):
        lanes = slice(h * half, (h + 1) * half)
        attended = ((whole[:, lanes] + own_num[h]) / total[:, lanes]).T.astype(BF16)
        for g in range(half // seqs):
            head = h * (half // seqs) + g
            att[:, pl.ds(head * hd, hd)] = attended[g * seqs : (g + 1) * seqs]

    local[9].wait()
    block = seqs // NZ
    width = w_v.shape[1] // CHUNKS
    relayed, plain, joined, across = {}, {}, {}, {}
    order = [k // 2 + (k % 2) * (CHUNKS // 2) for k in range(CHUNKS)]
    pl.semaphore_wait(diag_sem, 2)
    def piece_of(k):
        return jnp.dot(att[...], w_v[:, pl.ds(k * width, width)], preferred_element_type=F32).astype(BF16)

    piece = piece_of(order[0])
    for n, k in enumerate(order):
        via, other = (1, 3) if k < CHUNKS // 2 else (3, 1)
        cols = pl.ds(k * width, width)
        later = piece_of(order[n + 1]) if n + 1 < CHUNKS else None
        for i in range(NZ):
            for j in range(2):
                pz[i, j, :, cols] = piece[i * block + j * 8 : i * block + j * 8 + 8]
        piece = later

        def to_sum(src, dx, dz, n):
            slot = 4 if dz == 0 else 2 * dx + dz // 2
            return remote(src, zr.at[slot, :, cols], z_send.at[n], z_recv.at[CHUNKS + k], head_at(dx, dz))

        relayed[k] = remote(pz.at[(z + 2) % NZ, :, :, cols], zt.at[:, :, cols], z_send.at[0], z_recv.at[k], head_at(0, via))
        plain[k] = [to_sum(pz.at[(z + other) % NZ, (xl + dx) % 2, :, cols], dx, other, 1) for dx in range(2)]
        joined[k] = [to_sum(zj.at[(xl + dx) % 2, :, cols], dx, via, 2) for dx in range(2)]
        across[k] = [to_sum(pz.at[z, 1 - xl, :, cols], 1, 0, 3)]
        relayed[k].start()
    for k in order:
        for copy in (*plain[k], *across[k]):
            copy.start()
    for k in order:
        via = 1 if k < CHUNKS // 2 else 3
        cols = pl.ds(k * width, width)
        relayed[k].wait_recv()
        for j in range(2):
            zj[j, :, cols] = (pz[(z + via) % NZ, j, :, cols].astype(F32) + zt[j, :, cols].astype(F32)).astype(BF16)
        for copy in joined[k]:
            copy.start()
    square = jnp.zeros((block // 2, 1), F32)
    for k in order:
        cols = pl.ds(k * width, width)
        settle(zr.at[:, :, cols], z_recv.at[CHUNKS + k])
        projected = pz[z, xl, :, cols].astype(F32)
        for i in range(5):
            projected = projected + zr[i, :, cols].astype(F32)
        near_sum[:, cols] = projected
        square = square + jnp.sum(projected * projected, axis=1, keepdims=True)
    out_ref[...] = near_sum[...] / jnp.sqrt(square / w_v.shape[1] + epsilon)

    settle(hk.at[pl.ds(0, 2 * HOT_CAP)], kv_send)
    settle(qt.at[pl.ds(0, len(gathers))], ag_send)
    settle(ra, rs_send)
    settle(tot_ra, tot_send)
    for n in range(3):
        settle(zt, z_send.at[n])
    settle(zr.at[0], z_send.at[3])


def layer(queries, keys, values, hot_pages, hot_used, user_pages, lengths, o_weight):
    seqs, heads, hd = queries.shape
    pages, kvh, page, _ = keys.shape
    rows = seqs * heads
    width = o_weight.shape[1]
    vmem = pltpu.VMEM
    return pl.pallas_call(
        layer_kernel,
        out_shape=pltpu.VMEM((seqs // 8, width), F32),
        in_specs=[pl.BlockSpec(memory_space=pl.ANY)] * 8,
        out_specs=pl.BlockSpec(memory_space=pltpu.VMEM),
        scratch_shapes=[
            vmem((rows, hd), BF16),
            vmem((1, hot_pages.shape[0]), I32),
            vmem((hot_used.shape[0] // 128, 128), I32),
            vmem((1, seqs), I32),
            pltpu.SMEM((1, seqs), I32),
            vmem((pages - HOT_CAP, kvh, page, hd), BF16),
            vmem((pages - HOT_CAP, kvh, page, hd), BF16),
            vmem((2 * HOT_CAP, kvh, page, hd), BF16),
            vmem((2 * HOT_CAP, kvh, page, hd), BF16),
            vmem((kvh, hd, 2 * HOT_CAP * page), BF16),
            vmem((8, hd, rows), BF16),
            vmem((1, kvh * hd, rows), BF16),
            vmem((8, rows), F32),
            vmem((8, rows), F32),
            vmem((2 * HOT_CAP, 128), F32),
            vmem((2, 2 * HOT_CAP * page, rows), BF16),
            vmem((8, hd, rows), BF16),
            vmem((7, hd, rows), BF16),
            vmem((8, 1, rows), F32),
            vmem((7, 1, rows), F32),
            vmem((page, rows), F32),
            vmem((rows, page), F32),
            vmem((rows, kvh * hd), F32),
            vmem(o_weight.shape, BF16),
            vmem((seqs, heads * hd), BF16),
            vmem((NZ, 2, 8, width), BF16),
            vmem((2, 8, width), BF16),
            vmem((2, 8, width), BF16),
            vmem((5, 8, width), BF16),
            vmem((seqs // 8, width), F32),
            pltpu.SemaphoreType.DMA((10,)),
            pltpu.SemaphoreType.DMA((4,)),
            pltpu.SemaphoreType.DMA((2 * CHUNKS,)),
            pltpu.SemaphoreType.DMA,
            pltpu.SemaphoreType.DMA((2,)),
            pltpu.SemaphoreType.DMA,
            pltpu.SemaphoreType.DMA((7,)),
            pltpu.SemaphoreType.DMA,
            pltpu.SemaphoreType.DMA,
            pltpu.SemaphoreType.DMA,
            pltpu.SemaphoreType.DMA,
            pltpu.SemaphoreType.REGULAR,
            pltpu.SemaphoreType.REGULAR,
        ],
        compiler_params=pltpu.CompilerParams(
            collective_id=0, has_side_effects=True, vmem_limit_bytes=64_500_000
        ),
        name="layer",
    )(
        queries.reshape(rows, hd),
        keys,
        values,
        hot_pages.reshape(1, -1),
        hot_used.reshape(-1, 128),
        user_pages.reshape(1, -1),
        lengths.reshape(1, -1),
        o_weight,
    )


def per_device(
    queries, keys, values, hot_pages, hot_used, user_pages, lengths, o_weight, residual, norm_gain
):
    normed = layer(queries, keys, values, hot_pages, hot_used, user_pages, lengths, o_weight)
    return (residual.astype(F32) + normed * norm_gain[None, :]).astype(BF16)


def solution(mesh):
    in_specs = (
        P("pages", "heads", None),
        P("pages", "heads", None, None),
        P("pages", "heads", None, None),
        P(),
        P(),
        P("pages", None),
        P("pages"),
        P("heads", None),
        P(("pages", "heads"), None),
        P(),
    )
    out_specs = P(("pages", "heads"), None)
    return jax.shard_map(
        per_device, mesh=mesh, in_specs=in_specs, out_specs=out_specs, check_vma=False
    )
```

```python
import functools
import math

import jax
import jax.numpy as jnp
from jax import lax
from jax.experimental import pallas as pl
from jax.experimental.pallas import tpu as pltpu
from jax.sharding import PartitionSpec as P

HOT_CAP = 8
soft_cap = 50.0
score_scale = 1.0 / 12.0
epsilon = 1e-06
NY = 4
NZ = 4
CHUNKS = 6
F32, BF16, I32 = jnp.float32, jnp.bfloat16, jnp.int32
MESH = pl.DeviceIdType.MESH

A3, B0, A1, A2, B2, B1, B3, A0 = range(8)
OWNER = {A3: (3, 0), A1: (1, 0), A2: (2, 0), B0: (0, 1), B3: (3, 1), B1: (1, 1), B2: (2, 1), A0: (0, 0)}


def weights_of(logits):
    return jnp.exp2(jnp.tanh(logits * (score_scale / soft_cap)) * (soft_cap * math.log2(math.e)))


def layer_kernel(
    q_hbm, k_hbm, v_hbm, hot_hbm, used_hbm, up_hbm, len_hbm, w_hbm, out_ref,
    q_v, hot_v, used_v, len_v, up_s, kbuf, vbuf, hk, hv, vt, qt, qbd, urow, lrow, pos,
    wt, res, ra, tot, tot_ra, own_t, own_w, own_o,
    w_v, att, pz, zr, near_sum,
    in_sem, z_send, z_recv, kv_send, kv_recv, ag_send, ag_recv, rs_send, rs_recv, tot_send, tot_recv, far_sem, diag_sem,
):
    seqs = len_v.shape[1]
    kvh, page, hd = hk.shape[1:]
    rows = q_v.shape[0]
    half = rows // kvh
    me = lax.axis_index("pages")
    y, xh, core = me // 4, (me // 2) % 2, me % 2

    member = lax.axis_index("heads")
    xl, z = member // NZ, member % NZ

    def head_at(dx, dz):
        return {"heads": ((xl + dx) % 2) * NZ + (z + dz) % NZ}

    def seq_at(place):
        return ((place // 8) % 2) * (seqs // 2) + (place // 16) * 8 + place % 8

    def at(dy, dx=0, dc=0):
        return {"pages": ((y + dy) % NY) * 4 + ((xh + dx) % 2) * 2 + (core + dc) % 2}

    def remote(src, dst, send, recv, target):
        return pltpu.make_async_remote_copy(
            src_ref=src, dst_ref=dst, send_sem=send, recv_sem=recv, device_id=target, device_id_type=MESH
        )

    own = pl.ds(HOT_CAP, k_hbm.shape[0] - HOT_CAP)
    hot = pl.ds(0, HOT_CAP)
    def settle(like, semaphore):
        pltpu.make_async_copy(like, like, semaphore).wait()

    local = [
        pltpu.make_async_copy(q_hbm, q_v, in_sem.at[0]),
        pltpu.make_async_copy(hot_hbm, hot_v, in_sem.at[1]),
        pltpu.make_async_copy(used_hbm, used_v, in_sem.at[2]),
        pltpu.make_async_copy(len_hbm, len_v, in_sem.at[3]),
        pltpu.make_async_copy(up_hbm, up_s, in_sem.at[4]),
        pltpu.make_async_copy(k_hbm.at[hot], hk.at[hot], in_sem.at[5]),
        pltpu.make_async_copy(v_hbm.at[hot], hv.at[hot], in_sem.at[6]),
        pltpu.make_async_copy(k_hbm.at[own], kbuf, in_sem.at[7]),
        pltpu.make_async_copy(v_hbm.at[own], vbuf, in_sem.at[8]),
        pltpu.make_async_copy(w_hbm, w_v, in_sem.at[9]),
    ]
    for copy in local[:8]:
        copy.start()

    barrier = pltpu.get_barrier_semaphore()
    peers = [at(1), at(2), at(3), at(0, 1), at(0, 0, 1)]
    peers += [head_at(0, 1), head_at(0, 3), head_at(1, 0)]
    for peer in peers:
        pl.semaphore_signal(barrier, inc=1, device_id=peer, device_id_type=MESH)

    r = lax.broadcasted_iota(I32, (rows, rows), 0)
    col = lax.broadcasted_iota(I32, (rows, rows), 1)
    heads = rows // seqs
    perm = jnp.where(col == seq_at(r % seqs) * heads + r // seqs, 1.0, 0.0).astype(BF16)
    local[0].wait()
    q_rows = jnp.dot(perm, q_v[...], preferred_element_type=F32)
    qt[A0] = q_rows.T.astype(BF16)

    pl.semaphore_wait(barrier, len(peers))

    far = pl.ds(HOT_CAP, HOT_CAP)
    kv_copies = [
        remote(hk.at[hot], hk.at[far], kv_send, kv_recv.at[0], at(0, 0, 1)),
        remote(hv.at[hot], hv.at[far], kv_send, kv_recv.at[1], at(0, 0, 1)),
    ]
    gathers, returns = {}, {}
    for step, (dy, dx) in OWNER.items():
        if step == A0:
            continue
        back = next(k for k, at_ in OWNER.items() if at_ == ((NY - dy) % NY, dx))
        gathers[step] = remote(qt.at[A0], qt.at[step], ag_send, ag_recv.at[step], at((NY - dy) % NY, dx))
        returns[step] = [
            remote(res.at[step], ra.at[back], rs_send, rs_recv, at(dy, dx)),
            remote(tot.at[step], tot_ra.at[back], tot_send, tot_recv, at(dy, dx)),
        ]
    pl.semaphore_signal(far_sem, inc=1, device_id=at(0, 1), device_id_type=MESH)
    for dz in (1, 3):
        pl.semaphore_signal(diag_sem.at[0], inc=1, device_id=head_at(0, dz), device_id_type=MESH)
    for step in (B0, A3, A1, A2):
        gathers[step].start()
    local[5].wait()
    local[6].wait()
    kv_copies[0].start()
    local[8].start()
    local[9].start()

    for copy in local[1:5]:
        copy.wait()
    lane = lax.broadcasted_iota(I32, (2 * seqs, rows), 0)
    pick = seq_at(lax.broadcasted_iota(I32, (2 * seqs, rows), 1) % seqs)
    spread = jnp.where(lane == core * seqs + pick, 1.0, 0.0).astype(BF16)
    used = jnp.dot(used_v[...].astype(F32).astype(BF16), spread, preferred_element_type=F32)
    own_t[pl.ds(0, 8), :] = used
    for step, (dy, dx) in OWNER.items():
        chip = ((y + dy) % NY) * 2 + (xh + dx) % 2
        urow[pl.ds(step, 1), :] = own_t[pl.ds(chip, 1), :]
    lane = lax.broadcasted_iota(I32, (seqs, rows), 0)
    pick = seq_at(lax.broadcasted_iota(I32, (seqs, rows), 1) % seqs)
    spread = jnp.where(lane == pick, 1.0, 0.0).astype(BF16)
    lens = jnp.broadcast_to(len_v[...].astype(F32), (8, seqs)).astype(BF16)
    lrow[...] = jnp.dot(lens, spread, preferred_element_type=F32)
    hot_n = hot_v.shape[1]
    cand = lax.broadcasted_iota(I32, (2 * HOT_CAP, hot_n), 0)
    group = jnp.where(cand < HOT_CAP, me, at(0, 0, 1)["pages"])
    match = hot_v[...] == group * k_hbm.shape[0] + cand % HOT_CAP
    order = lax.broadcasted_iota(I32, (2 * HOT_CAP, hot_n), 1).astype(F32)
    pos[...] = jnp.broadcast_to(
        jnp.min(jnp.where(match, order, 1e9), axis=1, keepdims=True), pos.shape
    )

    qbd[...] = jnp.zeros_like(qbd)

    def set_queries(step):
        qbd[0, pl.ds(0, hd), pl.ds(0, half)] = qt[step, :, pl.ds(0, half)]
        qbd[0, pl.ds(hd, hd), pl.ds(half, half)] = qt[step, :, pl.ds(half, half)]

    def transpose_values(first):
        for j in range(first, first + HOT_CAP):
            for h in range(kvh):
                vt[h, :, pl.ds(j * page, page)] = hv[j, h].T

    transpose_values(0)

    def shared_block(step, slot, previous):
        if step is not None:
            set_queries(step)
            allowed = jnp.where(urow[pl.ds(step, 1), :] > pos[:, pl.ds(0, 1)], 1.0, 0.0)
            sums = jnp.zeros((8, rows), F32)
        parts = [jnp.zeros((hd, half), F32) for _ in range(kvh)]

        def scores(c):
            keys = jnp.concatenate(
                [hk[pl.ds(2 * c, 2), h].reshape(2 * page, hd) for h in range(kvh)], axis=1
            )
            return jnp.dot(keys, qbd[0], preferred_element_type=F32)

        def values(c):
            for h in range(kvh):
                parts[h] = parts[h] + jnp.dot(
                    vt[h, :, pl.ds(2 * c * page, 2 * page)],
                    wt[1 - slot, pl.ds(2 * c * page, 2 * page), pl.ds(h * half, half)],
                    preferred_element_type=F32,
                )

        if step is not None:
            logits = scores(0)
        for c in range(HOT_CAP):
            if previous is not None:
                values(c)
            if step is None:
                continue
            for i in range(2 * page // 16):
                j = (2 * c * page + i * 16) // page
                weight = weights_of(logits[i * 16 : (i + 1) * 16]) * allowed[j : j + 1]
                sums = sums + weight[:8] + weight[8:]
                wt[slot, pl.ds(2 * c * page + i * 16, 16), :] = weight.astype(BF16)
            if c + 1 < HOT_CAP:
                logits = scores(c + 1)
        if step is not None:
            tot[step] = jnp.sum(sums, axis=0, keepdims=True)
        if previous is not None:
            for h in range(kvh):
                res[previous, :, pl.ds(h * half, half)] = parts[h].astype(BF16)

    def page_of(place):
        return jnp.maximum(up_s[0, seq_at(place)] - HOT_CAP, 0)

    def own_scores(first, last):
        def some(g, carry):
            seq_of = lax.broadcasted_iota(I32, (page, rows), 1) % seqs
            tile = own_t[...]
            for i in range(0, 16, 2):
                pages = [page_of(g * 16 + i + j) for j in range(2)]
                keys = jnp.concatenate(
                    [jnp.concatenate([kbuf[u, h] for h in range(kvh)], axis=1) for u in pages], axis=0
                )
                logits = jnp.dot(keys, qbd[0], preferred_element_type=F32)
                for j in range(2):
                    tile = jnp.where(seq_of == g * 16 + i + j, logits[j * page : (j + 1) * page], tile)
            own_t[...] = tile
            return carry

        lax.fori_loop(first, last, some, 0)

    def own_weights():
        token = lax.broadcasted_iota(I32, (page, rows), 0).astype(F32)
        weight = jnp.where(token < lrow[pl.ds(0, 1), :], weights_of(own_t[...]), 0.0)
        own_t[pl.ds(0, 8), :] = jnp.broadcast_to(jnp.sum(weight, axis=0, keepdims=True), (8, rows))
        own_w[...] = weight.T

    def own_values():
        local[8].wait()

        def some(n, carry):
            row = lax.broadcasted_iota(I32, (8 * heads, page), 0) % 8
            for m in range(4):
                g = n * 4 + m
                weight = jnp.concatenate([own_w[pl.ds(h * seqs + g * 8, 8), :] for h in range(heads)], axis=0)
                left, right = [], []
                for i in range(8):
                    u = page_of(g * 8 + i)
                    left.append(jnp.where(row == i, weight, 0.0).astype(BF16))
                    right.append(jnp.concatenate([vbuf[u, h] for h in range(kvh)], axis=1))
                part = jnp.dot(
                    jnp.concatenate(left, axis=1), jnp.concatenate(right, axis=0), preferred_element_type=F32
                )
                for h in range(heads):
                    own_o[pl.ds(h * seqs + g * 8, 8), :] = part[h * 8 : (h + 1) * 8]
            return carry

        lax.fori_loop(0, seqs // 32, some, 0)

    set_queries(A0)
    own_t[...] = jnp.zeros_like(own_t)
    pl.semaphore_wait(far_sem, 1)
    for step in (B2, B1, B3):
        gathers[step].start()
    kv_copies[1].start()
    local[7].wait()
    own_scores(0, seqs // 64)
    kv_copies[0].wait_recv()

    def arrive(step, steps):
        for k in steps:
            @pl.when(step == k)
            def _():
                gathers[k].wait_recv()

    def send_back(step, steps):
        for k in steps:
            @pl.when(step == k)
            def _():
                for copy in returns[k]:
                    copy.start()

    def two_steps(n, carry):
        step = 2 * n + 1
        arrive(step, (1, 3, 5))
        shared_block(step, 1, step - 1)
        send_back(step - 1, (0, 2, 4))
        arrive(step + 1, (2, 4, 6))
        shared_block(step + 1, 0, step)
        send_back(step, (1, 3, 5))
        return carry

    gathers[0].wait_recv()
    shared_block(0, 0, None)
    kv_copies[1].wait_recv()
    transpose_values(HOT_CAP)
    lax.fori_loop(0, 3, two_steps, 0)
    shared_block(None, 1, 6)
    for copy in returns[6]:
        copy.start()
    shared_block(7, 1, None)
    shared_block(None, 0, 7)
    pl.semaphore_wait(diag_sem.at[0], 2)
    pl.semaphore_signal(diag_sem.at[1], inc=1, device_id=head_at(1, 0), device_id_type=MESH)
    own_scores(seqs // 64, seqs // 16)
    own_weights()
    own_values()

    def summed(pieces):
        return sum(piece[...].astype(F32) for piece in pieces)

    own_num = [own_o[pl.ds(h * half, half), pl.ds(h * hd, hd)].T for h in range(kvh)]
    settle(ra, rs_recv)
    settle(tot_ra, tot_recv)
    whole = summed([res.at[A0], *(ra.at[k] for k in returns)])
    total = sum((tot_ra[k] for k in returns), tot[A0]) + own_t[pl.ds(0, 1), :]
    for h in range(kvh):
        lanes = slice(h * half, (h + 1) * half)
        attended = ((whole[:, lanes] + own_num[h]) / total[:, lanes]).T.astype(BF16)
        for g in range(half // seqs):
            head = h * (half // seqs) + g
            att[:, pl.ds(head * hd, hd)] = attended[g * seqs : (g + 1) * seqs]

    local[9].wait()
    block = seqs // NZ
    width = w_v.shape[1] // CHUNKS
    pl.semaphore_wait(diag_sem.at[1], 1)
    def piece_of(k):
        return jnp.dot(att[...], w_v[:, pl.ds(k * width, width)], preferred_element_type=F32).astype(BF16)

    piece = piece_of(0)
    for k in range(CHUNKS):
        cols = pl.ds(k * width, width)
        later = piece_of(k + 1) if k + 1 < CHUNKS else None
        for i in range(NZ):
            for j in range(2):
                pz[i, j, :, cols] = piece[i * block + j * 8 : i * block + j * 8 + 8]
        piece = later
        for dz in (2, 1, 3, 0):
            for dx in range(2):
                if dz == 0 and dx == 0:
                    continue
                src = pz.at[(z + dz) % NZ, (xl + dx) % 2, :, cols]
                slot = dx * NZ + dz - 1
                remote(src, zr.at[slot, :, cols], z_send, z_recv.at[k], head_at(dx, dz)).start()
    square = jnp.zeros((block // 2, 1), F32)
    for k in range(CHUNKS):
        cols = pl.ds(k * width, width)
        settle(zr.at[:, :, cols], z_recv.at[k])
        projected = pz[z, xl, :, cols].astype(F32)
        for i in range(2 * NZ - 1):
            projected = projected + zr[i, :, cols].astype(F32)
        near_sum[:, cols] = projected
        square = square + jnp.sum(projected * projected, axis=1, keepdims=True)
    out_ref[...] = near_sum[...] / jnp.sqrt(square / w_v.shape[1] + epsilon)

    settle(hk.at[pl.ds(0, 2 * HOT_CAP)], kv_send)
    settle(qt.at[pl.ds(0, len(gathers))], ag_send)
    settle(ra, rs_send)
    settle(tot_ra, tot_send)
    settle(zr, z_send)


def layer(queries, keys, values, hot_pages, hot_used, user_pages, lengths, o_weight):
    seqs, heads, hd = queries.shape
    pages, kvh, page, _ = keys.shape
    rows = seqs * heads
    width = o_weight.shape[1]
    vmem = pltpu.VMEM
    return pl.pallas_call(
        layer_kernel,
        out_shape=pltpu.VMEM((seqs // 8, width), F32),
        in_specs=[pl.BlockSpec(memory_space=pl.ANY)] * 8,
        out_specs=pl.BlockSpec(memory_space=pltpu.VMEM),
        scratch_shapes=[
            vmem((rows, hd), BF16),
            vmem((1, hot_pages.shape[0]), I32),
            vmem((hot_used.shape[0] // 128, 128), I32),
            vmem((1, seqs), I32),
            pltpu.SMEM((1, seqs), I32),
            vmem((pages - HOT_CAP, kvh, page, hd), BF16),
            vmem((pages - HOT_CAP, kvh, page, hd), BF16),
            vmem((2 * HOT_CAP, kvh, page, hd), BF16),
            vmem((2 * HOT_CAP, kvh, page, hd), BF16),
            vmem((kvh, hd, 2 * HOT_CAP * page), BF16),
            vmem((8, hd, rows), BF16),
            vmem((1, kvh * hd, rows), BF16),
            vmem((8, rows), F32),
            vmem((8, rows), F32),
            vmem((2 * HOT_CAP, 128), F32),
            vmem((2, 2 * HOT_CAP * page, rows), BF16),
            vmem((8, hd, rows), BF16),
            vmem((7, hd, rows), BF16),
            vmem((8, 1, rows), F32),
            vmem((7, 1, rows), F32),
            vmem((page, rows), F32),
            vmem((rows, page), F32),
            vmem((rows, kvh * hd), F32),
            vmem(o_weight.shape, BF16),
            vmem((seqs, heads * hd), BF16),
            vmem((NZ, 2, 8, width), BF16),
            vmem((2 * NZ - 1, 8, width), BF16),
            vmem((seqs // 8, width), F32),
            pltpu.SemaphoreType.DMA((10,)),
            pltpu.SemaphoreType.DMA,
            pltpu.SemaphoreType.DMA((CHUNKS,)),
            pltpu.SemaphoreType.DMA,
            pltpu.SemaphoreType.DMA((2,)),
            pltpu.SemaphoreType.DMA,
            pltpu.SemaphoreType.DMA((7,)),
            pltpu.SemaphoreType.DMA,
            pltpu.SemaphoreType.DMA,
            pltpu.SemaphoreType.DMA,
            pltpu.SemaphoreType.DMA,
            pltpu.SemaphoreType.REGULAR,
            pltpu.SemaphoreType.REGULAR((2,)),
        ],
        compiler_params=pltpu.CompilerParams(
            collective_id=0, has_side_effects=True, vmem_limit_bytes=64_500_000
        ),
        name="layer",
    )(
        queries.reshape(rows, hd),
        keys,
        values,
        hot_pages.reshape(1, -1),
        hot_used.reshape(-1, 128),
        user_pages.reshape(1, -1),
        lengths.reshape(1, -1),
        o_weight,
    )


def per_device(
    queries, keys, values, hot_pages, hot_used, user_pages, lengths, o_weight, residual, norm_gain
):
    normed = layer(queries, keys, values, hot_pages, hot_used, user_pages, lengths, o_weight)
    return (residual.astype(F32) + normed * norm_gain[None, :]).astype(BF16)


def solution(mesh):
    in_specs = (
        P("pages", "heads", None),
        P("pages", "heads", None, None),
        P("pages", "heads", None, None),
        P(),
        P(),
        P("pages", None),
        P("pages"),
        P("heads", None),
        P(("pages", "heads"), None),
        P(),
    )
    out_specs = P(("pages", "heads"), None)
    return jax.shard_map(
        per_device, mesh=mesh, in_specs=in_specs, out_specs=out_specs, check_vma=False
    )
```
